32 devices in a mesh: data: 32 (over z, y, x, core).
Axes of the slice: x: 2, y: 2, z: 4, core: 2. Of those that a mesh axis runs over, the one named last changes fastest.
Arguments:
- tokens: bfloat16 [16384, 384], P('data')
- w_in: bfloat16 [384, 1536], replicated
- w_out: bfloat16 [1536, 384], replicated
- task_heads: bfloat16 [3, 384, 13], replicated
- labels: int32 [3, 16384], P(None, 'data')
- label_mask: int32 [3, 16384], P(None, 'data')
Outputs:
- output 1: float32 [3], replicated
- output 2: float32 [589824], P('data')
- output 3: float32 [589824], P('data')
All inputs are finite; a program needn't handle non-finite values.
Results may differ from the reference program's by a relative error of at most 0.00270601.
Values are sent between devices in bfloat16 or wider.
A program may use at most 1 GiB of HBM per device.

```python
import jax
import jax.numpy as jnp
from jax import lax

MODEL_DIM = 384
HIDDEN_DIM = 1536
NUM_TASKS = 3
NUM_CLASSES = 13
TOK_DEV = 512
GROUP_SIZE = 32
SOLVER_STEPS = 20


def draw_labels(rng_key):
    sub_keys = jax.random.split(rng_key, 7)
    tokens_total = TOK_DEV * GROUP_SIZE
    dev_class = jax.random.randint(sub_keys[0], (GROUP_SIZE, 1), 0, NUM_CLASSES)
    keep_draw = jax.random.randint(sub_keys[1], (GROUP_SIZE, TOK_DEV), 0, 4)
    free_class = jax.random.randint(sub_keys[2], (GROUP_SIZE, TOK_DEV), 0, NUM_CLASSES)
    common_class = jnp.where(keep_draw < 3, dev_class, free_class).reshape(tokens_total)
    noise_draw = jax.random.randint(sub_keys[3], (NUM_TASKS, tokens_total), 0, 4)
    task_class = jax.random.randint(sub_keys[4], (NUM_TASKS, tokens_total), 0, NUM_CLASSES)
    labels = jnp.where(noise_draw == 0, task_class, common_class[None, :]).astype(jnp.int32)
    mask_level = jax.random.randint(sub_keys[5], (NUM_TASKS, GROUP_SIZE, 1), 5, 100)
    mask_draw = jax.random.randint(sub_keys[6], (NUM_TASKS, GROUP_SIZE, TOK_DEV), 0, 100)
    label_mask = (mask_draw < mask_level).astype(jnp.int32).reshape(NUM_TASKS, tokens_total)
    return labels, label_mask


def setup_inputs(seed: int = 0) -> dict:
    rng_keys = jax.random.split(jax.random.key(seed), 6)
    tokens_total = TOK_DEV * GROUP_SIZE
    tokens = jax.random.normal(rng_keys[0], (tokens_total, MODEL_DIM), jnp.float32)
    w_in = jax.random.normal(rng_keys[1], (MODEL_DIM, HIDDEN_DIM), jnp.float32) * MODEL_DIM ** -0.5
    w_out = jax.random.normal(rng_keys[2], (HIDDEN_DIM, MODEL_DIM), jnp.float32) * HIDDEN_DIM ** -0.5
    shared_head = jax.random.normal(rng_keys[3], (MODEL_DIM, NUM_CLASSES), jnp.float32)
    own_head = jax.random.normal(rng_keys[4], (NUM_TASKS, MODEL_DIM, NUM_CLASSES), jnp.float32)
    head_sign = (1 - 2 * (jnp.arange(NUM_TASKS) % 2)).astype(jnp.float32)
    task_heads = (head_sign[:, None, None] * shared_head[None] + 0.6 * own_head) * (1.5 * MODEL_DIM ** -0.5)
    labels, label_mask = draw_labels(rng_keys[5])
    return {"tokens": tokens.astype(jnp.bfloat16), "w_in": w_in.astype(jnp.bfloat16), "w_out": w_out.astype(jnp.bfloat16), "task_heads": task_heads.astype(jnp.bfloat16), "labels": labels, "label_mask": label_mask}


def device_grads(x_loc, w_in, w_out, task_heads, lab_loc, mask_loc):
    pre_act = jnp.dot(x_loc, w_in, preferred_element_type=jnp.float32)
    act_out, gelu_slope = jax.jvp(jax.nn.gelu, (pre_act,), (jnp.ones_like(pre_act),))
    act_bf = act_out.astype(jnp.bfloat16)
    residual = x_loc.astype(jnp.float32) + jnp.dot(act_bf, w_out, preferred_element_type=jnp.float32)
    z_bf = residual.astype(jnp.bfloat16)
    heads_wide = task_heads.astype(jnp.float32)
    logits = jnp.einsum("bd,tdc->tbc", z_bf.astype(jnp.float32), heads_wide)
    soft_prob = jax.nn.softmax(logits, axis=-1)
    onehot = (lab_loc[:, :, None] == jnp.arange(NUM_CLASSES)[None, None, :]).astype(jnp.float32)
    d_logit = (mask_loc[:, :, None].astype(jnp.float32) * (soft_prob - onehot)).astype(jnp.bfloat16)
    d_resid = jnp.einsum("tbc,tdc->tbd", d_logit.astype(jnp.float32), heads_wide).astype(jnp.bfloat16)
    d_wide = d_resid.astype(jnp.float32)
    grad_w_out = jnp.einsum("bf,tbd->tfd", act_bf.astype(jnp.float32), d_wide)
    d_act = jnp.einsum("tbd,fd->tbf", d_wide, w_out.astype(jnp.float32))
    d_pre = (d_act * gelu_slope[None]).astype(jnp.bfloat16)
    grad_w_in = jnp.einsum("bd,tbf->tdf", x_loc.astype(jnp.float32), d_pre.astype(jnp.float32))
    return grad_w_in, grad_w_out


def solve_weights(gram_mat):
    step_scale = jnp.trace(gram_mat) / NUM_TASKS

    def solver_step(step_idx, weights):
        pull_vec = (gram_mat * weights[None, :]).sum(axis=1)
        raised = weights * jnp.exp(-pull_vec / step_scale)
        return raised / raised.sum()

    init_weights = jnp.full((NUM_TASKS,), 1.0 / NUM_TASKS, jnp.float32)
    return lax.fori_loop(0, SOLVER_STEPS, solver_step, init_weights)


def reference(tokens, w_in, w_out, task_heads, labels, label_mask):
    inv_count = 1.0 / jnp.maximum(label_mask.sum(axis=1), 1).astype(jnp.float32)
    tok_blocks = tokens.reshape(GROUP_SIZE, TOK_DEV, MODEL_DIM)
    lab_blocks = labels.reshape(NUM_TASKS, GROUP_SIZE, TOK_DEV).transpose(1, 0, 2)
    mask_blocks = label_mask.reshape(NUM_TASKS, GROUP_SIZE, TOK_DEV).transpose(1, 0, 2)
    flat_len = MODEL_DIM * HIDDEN_DIM

    def add_device(grad_sum, block_in):
        x_loc, lab_loc, mask_loc = block_in
        grad_w_in, grad_w_out = device_grads(x_loc, w_in, w_out, task_heads, lab_loc, mask_loc)
        flat_grad = jnp.concatenate([grad_w_in.reshape(NUM_TASKS, flat_len), grad_w_out.reshape(NUM_TASKS, flat_len)], axis=1)
        part_grad = (flat_grad * inv_count[:, None]).astype(jnp.bfloat16).astype(jnp.float32)
        return grad_sum + part_grad, None

    grad_sum, _ = lax.scan(add_device, jnp.zeros((NUM_TASKS, 2 * flat_len), jnp.float32), (tok_blocks, lab_blocks, mask_blocks))
    gram_mat = jnp.dot(grad_sum, grad_sum.T, preferred_element_type=jnp.float32)
    weights = solve_weights(gram_mat)
    combined = (weights[:, None] * grad_sum).sum(axis=0)
    return weights, combined[:flat_len], combined[flat_len:]
```

```python
import jax
import jax.numpy as jnp
from jax import lax
from jax.experimental import pallas as pl
from jax.experimental.pallas import tpu as pltpu
from jax.sharding import PartitionSpec as P

MESH = pl.DeviceIdType.MESH
SOLVER_STEPS = 20
N_DEV = 32
TOK, DIM, HID, TASKS, CLS, PAD = 512, 384, 1536, 3, 13, 16
ZA, ZB = 16, 8
CHUNKS = 4
ROWS = DIM // CHUNKS
GELU_C = 0.7978845608028654
GELU_A = 0.044715
N_SEM = 48

F32, BF16 = jnp.float32, jnp.bfloat16


def dot(a, b):
    return jnp.dot(a, b, preferred_element_type=F32)


def dot_nt(a, b):
    return lax.dot_general(a, b, (((1,), (1,)), ((), ())), preferred_element_type=F32)


def gelu_cdf(p):
    sq = p * p
    t = jnp.tanh(GELU_C * (p + GELU_A * (sq * p)))
    return sq, t, 0.5 * (1.0 + t)


def kernel(x_ref, w1_ref, w2_ref, hp_ref, lab_ref, msk_ref, al_ref, o1_ref, o2_ref,
           cnts, grams, gx, ge, ht, w1s, w2s, a_own, a_t, gp, dz, qt, inv, acc1, acc2,
           rc1, rc2, ra1, ra2, rb1, rb2, g1s, g2s, sb, rb,
           ss, rs, cs, cr, gs, gr):
    me = lax.axis_index("data")
    c = lax.rem(me, 2)
    x = lax.rem(me // 2, 2)
    y = lax.rem(me // 4, 2)
    za = lax.rem(me // ZA, 2)
    zb = lax.rem(me // ZB, 2)
    to_c = me + (1 - 2 * c)
    to_x = me + 2 * (1 - 2 * x)
    to_y = me + 4 * (1 - 2 * y)
    to_za = me + ZA * (1 - 2 * za)
    to_zb = me + ZB * (1 - 2 * zb)

    used = []

    def rcopy(src, dst, dev):
        i = len(used)
        used.append(i)
        return pltpu.make_async_remote_copy(src_ref=src, dst_ref=dst, send_sem=ss.at[i], recv_sem=rs.at[i],
                                            device_id=(dev,), device_id_type=MESH)

    pending = []

    def start(cp):
        cp.start()
        pending.append(cp)
        return cp

    def row_copy(buf, src_row, send_sem, recv_sem, dev):
        return pltpu.make_async_remote_copy(src_ref=buf.at[src_row], dst_ref=buf.at[src_row], send_sem=send_sem,
                                            recv_sem=recv_sem, device_id=(dev,), device_id_type=MESH)

    def exchange_start(buf, s_sem, r_sem):
        def go(i, _):
            row_copy(buf, me, s_sem.at[i], r_sem.at[me], lax.rem(me + i, N_DEV)).start()
            return 0
        lax.fori_loop(1, N_DEV, go, 0)

    def exchange_wait(buf, s_sem, r_sem):
        def go(i, _):
            peer = lax.rem(me + i, N_DEV)
            row_copy(buf, me, s_sem.at[i], r_sem.at[me], peer).wait_send()
            row_copy(buf, peer, s_sem.at[i], r_sem.at[peer], peer).wait_recv()
            return 0
        lax.fori_loop(1, N_DEV, go, 0)

    bar = pltpu.get_barrier_semaphore()

    def sig(i, _):
        pl.semaphore_signal(bar, inc=1, device_id=(lax.rem(me + i, N_DEV),), device_id_type=MESH)
        return 0
    lax.fori_loop(1, N_DEV, sig, 0)

    col = lax.broadcasted_iota(jnp.int32, (DIM, 1), 0)
    blk = (col * 43691) >> 19
    off = col - 12 * blk
    dev = (((blk >> 4) & 1) + 4 * ((blk >> 3) & 1) + ZB * ((blk >> 2) & 1) + ZA * ((blk >> 1) & 1) + 2 * (blk & 1))
    perm = (lax.broadcasted_iota(jnp.int32, (DIM, DIM), 1) == 12 * dev + off).astype(BF16)
    gx[0] = dot_nt(perm, x_ref[...]).astype(BF16)
    lane = lax.broadcasted_iota(jnp.int32, (1, 128), 1)
    row = jnp.zeros((1, 128), F32)
    for t in range(TASKS):
        row = row + jnp.where(lane == t, jnp.sum(msk_ref[t:t + 1, :].astype(F32), axis=1, keepdims=True), 0.0)
    cnts[me] = row

    pl.semaphore_wait(bar, N_DEV - 1)

    def chunk(k):
        return pl.ds(k * ROWS, ROWS)
    to_2 = [start(rcopy(gx.at[0, chunk(k)], gx.at[2, chunk(k)], to_za)) for k in range(CHUNKS)]
    to_1 = [start(rcopy(gx.at[0, chunk(k)], gx.at[1, chunk(k)], to_x)) for k in range(CHUNKS)]
    exchange_start(cnts, cs, cr)
    to_3 = [rcopy(gx.at[2, chunk(k)], gx.at[3, chunk(k)], to_x) for k in range(CHUNKS)]
    e_2 = rcopy(ge.at[0], ge.at[2], to_za)
    e_1 = rcopy(ge.at[0], ge.at[1], to_x)
    e_3 = rcopy(ge.at[2], ge.at[3], to_x)

    def fwd(i, _):
        cols = pl.ds(pl.multiple_of(i * 256, 256), 256)
        p = dot(x_ref[...], w1_ref[:, cols])
        a_own[:, cols] = (p * gelu_cdf(p)[2]).astype(BF16)
        return 0
    lax.fori_loop(0, HID // 256, fwd, 0)
    z = (x_ref[...].astype(F32) + dot(a_own[...], w2_ref[...])).astype(BF16)
    logits = dot_nt(hp_ref[...], z)
    cls = lax.broadcasted_iota(jnp.int32, (PAD, TOK), 0)
    valid = cls < CLS
    for t in range(TASKS):
        lg = jnp.where(valid, logits[PAD * t:PAD * (t + 1)], -jnp.inf)
        ex = jnp.exp(lg - jnp.max(lg, axis=0, keepdims=True))
        sm = ex / jnp.sum(ex, axis=0, keepdims=True)
        hot = (lab_ref[t:t + 1, :] == cls).astype(F32)
        ge[0, t] = jnp.where(valid, msk_ref[t:t + 1, :].astype(F32) * (sm - hot), 0.0).astype(BF16)
    start(e_2)
    start(e_1)

    seg = (col * 43691) >> 21
    src = 48 * (((seg >> 2) & 1) + ZB * ((seg >> 1) & 1) + 4 * (seg & 1) + ZA * za + 2 * x) + (col - 48 * seg)
    sel = (lax.broadcasted_iota(jnp.int32, (DIM, HID), 1) == src).astype(BF16)
    w1_rows = dot_nt(sel, w1_ref[...]).astype(BF16)
    w1s[...] = dot_nt(w1_rows, perm).astype(BF16)
    for k in range(8):
        dv = ((k >> 2) & 1) + ZB * ((k >> 1) & 1) + 4 * (k & 1) + ZA * za + 2 * x
        w2s[48 * k:48 * (k + 1), :] = w2_ref[pl.ds(pl.multiple_of(48 * dv, 16), 48), :]
    for t in range(TASKS):
        ht[t] = jnp.transpose(hp_ref[PAD * t:PAD * (t + 1), :].astype(F32)).astype(BF16)

    def acts(s):
        for r in range(3):
            rows = slice(128 * r, 128 * (r + 1))
            p = dot(w1s[rows, :], gx[s])
            sq, t, cdf = gelu_cdf(p)
            a_t[rows, :] = (p * cdf).astype(BF16)
            gp[rows, :] = cdf + (0.5 * GELU_C) * p * (1.0 - t * t) * (1.0 + (3.0 * GELU_A) * sq)

    def grads(s, t, first):
        dz[...] = dot(ht[t], ge[s, t]).astype(BF16)
        for r in range(3):
            rows = slice(128 * r, 128 * (r + 1))
            qt[rows, :] = (dot(w2s[rows, :], dz[...]) * gp[rows, :]).astype(BF16)
        sc = inv[t]
        d1 = (dot_nt(gx[s], qt[...]) * sc).astype(BF16).astype(F32)
        acc1[t] = d1 if first else acc1[t] + d1
        d2 = (dot_nt(a_t[...], dz[...]) * sc).astype(BF16).astype(F32)
        acc2[t] = d2 if first else acc2[t] + d2

    acts(0)
    to_2[0].wait_recv()
    start(to_3[0])
    exchange_wait(cnts, cs, cr)
    total = jnp.sum(cnts[...], axis=0)
    recip = 1.0 / jnp.maximum(total, 1.0)
    for t in range(TASKS):
        inv[t] = jnp.broadcast_to(recip[:, t:t + 1], (1, DIM))
    for t in range(TASKS):
        grads(0, t, True)
    to_2[1].wait_recv()
    start(to_3[1])
    for cp in to_1:
        cp.wait_recv()
    acts(1)
    e_1.wait_recv()
    to_2[2].wait_recv()
    start(to_3[2])
    for t in range(TASKS):
        grads(1, t, False)
    to_2[3].wait_recv()
    start(to_3[3])
    e_2.wait_recv()
    start(e_3)
    acts(2)
    for t in range(TASKS):
        grads(2, t, False)
    for cp in to_3:
        cp.wait_recv()
    acts(3)
    e_3.wait_recv()

    def rows_of(base, n):
        return pl.ds(pl.multiple_of(base, 48), n)
    c1, c2 = [], []
    for t in range(TASKS):
        grads(3, t, False)
        c1.append(start(rcopy(acc1.at[t, rows_of(192 * (1 - c), 192)], rc1.at[t], to_c)))
        c2.append(start(rcopy(acc2.at[t, rows_of(192 * (1 - c), 192)], rc2.at[t], to_c)))
    b0 = 192 * c
    h1, h2 = [], []
    for t in range(TASKS):
        c1[t].wait_recv()
        mine = rows_of(b0, 192)
        acc1[t, mine] = acc1[t, mine] + rc1[t]
        h1.append(start(rcopy(acc1.at[t, rows_of(b0 + 96 * (1 - y), 96)], ra1.at[t], to_y)))
        c2[t].wait_recv()
        acc2[t, mine] = acc2[t, mine] + rc2[t]
        h2.append(start(rcopy(acc2.at[t, rows_of(b0 + 96 * (1 - zb), 96)], ra2.at[t], to_zb)))
    q1, q2 = [], []
    for t in range(TASKS):
        h1[t].wait_recv()
        mine = rows_of(b0 + 96 * y, 96)
        acc1[t, mine] = acc1[t, mine] + ra1[t]
        q1.append(start(rcopy(acc1.at[t, rows_of(b0 + 96 * y + 48 * (1 - zb), 48)], rb1.at[t], to_zb)))
        h2[t].wait_recv()
        mine = rows_of(b0 + 96 * zb, 96)
        acc2[t, mine] = acc2[t, mine] + ra2[t]
        q2.append(start(rcopy(acc2.at[t, rows_of(b0 + 96 * zb + 48 * (1 - y), 48)], rb2.at[t], to_y)))
    own = 2 * za + x
    zero4 = jnp.zeros((4, DIM), F32)
    for t in range(TASKS):
        q1[t].wait_recv()
        g = acc1[t, rows_of(b0 + 96 * y + 48 * zb, 48)] + rb1[t]
        g1s[t] = g
        for k in range(4):
            sb[k, t] = jnp.concatenate([g[12 * k:12 * (k + 1)], zero4], axis=0)
        q2[t].wait_recv()
        g2s[t] = acc2[t, rows_of(b0 + 96 * zb + 48 * y, 48)] + rb2[t]

    row = jnp.zeros((1, 128), F32)
    pairs = [(0, 0), (0, 1), (0, 2), (1, 1), (1, 2), (2, 2)]
    for i, (t, s) in enumerate(pairs):
        part = jnp.sum(g1s[t] * g1s[s] + g2s[t] * g2s[s], axis=0, keepdims=True)
        row = row + jnp.where(lane == i, jnp.sum(part, axis=1, keepdims=True), 0.0)
    grams[me] = row
    exchange_start(grams, gs, gr)
    fx, fz = 1 - 2 * x, 2 * (1 - 2 * za)
    back = []
    for dk, to in ((fx, to_x), (fz, to_za), (fx + fz, to_x + to_za - me)):
        back.append(start(rcopy(sb.at[own + dk], rb.at[own], to)))
    rb[own] = sb[own]
    exchange_wait(grams, gs, gr)
    m = jnp.sum(grams[...], axis=0)
    ent = [m[:, i:i + 1] for i in range(6)]
    gram = {}
    for i, (t, s) in enumerate(pairs):
        gram[t, s] = gram[s, t] = ent[i]
    scale = (ent[0] + ent[3] + ent[5]) / TASKS

    def solve(_, w):
        up = []
        for t in range(TASKS):
            pull = gram[t, 0] * w[0] + gram[t, 1] * w[1] + gram[t, 2] * w[2]
            up.append(w[t] * jnp.exp(-pull / scale))
        tot = up[0] + up[1] + up[2]
        return tuple(u / tot for u in up)
    first = jnp.full((1, 1), 1.0 / TASKS, F32)
    w = lax.fori_loop(0, SOLVER_STEPS, solve, (first, first, first))
    al_ref[...] = jnp.concatenate(w, axis=1)
    gg = w[0] * g2s[0] + w[1] * g2s[1] + w[2] * g2s[2]
    for k in range(3):
        o2_ref[pl.ds(k, 48, stride=3), :] = gg[:, 128 * k:128 * (k + 1)]
    for cp in back:
        cp.wait_recv()
    for k in range(4):
        o1_ref[k] = w[0] * rb[k, 0] + w[1] * rb[k, 1] + w[2] * rb[k, 2]
    for cp in pending:
        cp.wait_send()


def solution(mesh):
    def step(tokens, w_in, w_out, heads, lab, msk):
        hp = jnp.pad(heads.transpose(0, 2, 1), ((0, 0), (0, PAD - CLS), (0, 0))).reshape(TASKS * PAD, DIM)
        vm = pl.BlockSpec(memory_space=pltpu.VMEM)
        dma = pltpu.SemaphoreType.DMA
        alpha, o1, o2 = pl.pallas_call(
            kernel,
            name="step",
            out_shape=(jax.ShapeDtypeStruct((1, TASKS), F32), jax.ShapeDtypeStruct((4, 16, DIM), F32),
                       jax.ShapeDtypeStruct((144, 128), F32)),
            in_specs=[vm] * 6,
            out_specs=(vm, vm, vm),
            scratch_shapes=[
                pltpu.VMEM((N_DEV, 1, 128), F32), pltpu.VMEM((N_DEV, 1, 128), F32),
                pltpu.VMEM((4, DIM, TOK), BF16), pltpu.VMEM((4, TASKS, PAD, TOK), BF16),
                pltpu.VMEM((TASKS, DIM, PAD), BF16), pltpu.VMEM((DIM, DIM), BF16), pltpu.VMEM((DIM, DIM), BF16),
                pltpu.VMEM((TOK, HID), BF16), pltpu.VMEM((DIM, TOK), BF16), pltpu.VMEM((DIM, TOK), F32),
                pltpu.VMEM((DIM, TOK), BF16), pltpu.VMEM((DIM, TOK), BF16), pltpu.VMEM((TASKS, 1, DIM), F32),
                pltpu.VMEM((TASKS, DIM, DIM), F32), pltpu.VMEM((TASKS, DIM, DIM), F32),
                pltpu.VMEM((TASKS, 192, DIM), F32), pltpu.VMEM((TASKS, 192, DIM), F32),
                pltpu.VMEM((TASKS, 96, DIM), F32), pltpu.VMEM((TASKS, 96, DIM), F32),
                pltpu.VMEM((TASKS, 48, DIM), F32), pltpu.VMEM((TASKS, 48, DIM), F32),
                pltpu.VMEM((TASKS, 48, DIM), F32), pltpu.VMEM((TASKS, 48, DIM), F32),
                pltpu.VMEM((4, TASKS, 16, DIM), F32), pltpu.VMEM((4, TASKS, 16, DIM), F32),
                dma((N_SEM,)), dma((N_SEM,)), dma((N_DEV,)), dma((N_DEV,)), dma((N_DEV,)), dma((N_DEV,)),
            ],
            compiler_params=pltpu.CompilerParams(collective_id=0, has_side_effects=True, vmem_limit_bytes=56 * 2**20),
        )(tokens, w_in, w_out, hp, lab, msk)
        g = o1[:, :12].reshape(2, 2, 12, 2, 2, 2, 48).transpose(2, 0, 4, 5, 1, 3, 6).reshape(-1)
        return alpha.reshape(TASKS), g, o2.reshape(-1)

    return jax.shard_map(step, mesh=mesh, in_specs=(P("data", None), P(), P(), P(), P(None, "data"), P(None, "data")),
                         out_specs=(P(), P("data"), P("data")), check_vma=False)
```

```python
import jax
import jax.numpy as jnp
from jax import lax
from jax.experimental import pallas as pl
from jax.experimental.pallas import tpu as pltpu
from jax.sharding import PartitionSpec as P

MESH = pl.DeviceIdType.MESH
SOLVER_STEPS = 20
N_DEV = 32
TOK, DIM, HID, TASKS, CLS, PAD = 512, 384, 1536, 3, 13, 16
ZA, ZB = 16, 8
CHUNKS = 4
ROWS = DIM // CHUNKS
GELU_C = 0.7978845608028654
GELU_A = 0.044715
N_SEM = 48

F32, BF16 = jnp.float32, jnp.bfloat16


def dot(a, b):
    return jnp.dot(a, b, preferred_element_type=F32)


def dot_nt(a, b):
    return lax.dot_general(a, b, (((1,), (1,)), ((), ())), preferred_element_type=F32)


def gelu_cdf(p):
    sq = p * p
    t = jnp.tanh(GELU_C * (p + GELU_A * (sq * p)))
    return sq, t, 0.5 * (1.0 + t)


def kernel(x_hbm, w1_hbm, w2_hbm, h_hbm, lab_hbm, msk_hbm, al_ref, o1_ref, o2_ref,
           x_ref, w1_ref, w2_ref, h_ref, lab_ref, msk_ref, hp_ref, cnts, grams, gx, ge, ht, w1s, w2s, a_own, a_t, gp, dz, qt, inv, acc1, acc2,
           rc1, rc2, ra1, ra2, rb1, rb2, g1s, g2s, sb, rb,
           ss, rs, cs, cr, gs, gr, ls):
    me = lax.axis_index("data")
    c = lax.rem(me, 2)
    x = lax.rem(me // 2, 2)
    y = lax.rem(me // 4, 2)
    za = lax.rem(me // ZA, 2)
    zb = lax.rem(me // ZB, 2)
    to_c = me + (1 - 2 * c)
    to_x = me + 2 * (1 - 2 * x)
    to_y = me + 4 * (1 - 2 * y)
    to_za = me + ZA * (1 - 2 * za)
    to_zb = me + ZB * (1 - 2 * zb)

    used = []

    def rcopy(src, dst, dev):
        i = len(used)
        used.append(i)
        return pltpu.make_async_remote_copy(src_ref=src, dst_ref=dst, send_sem=ss.at[i], recv_sem=rs.at[i],
                                            device_id=(dev,), device_id_type=MESH)

    pending = []

    def start(cp):
        cp.start()
        pending.append(cp)
        return cp

    def row_copy(buf, src_row, send_sem, recv_sem, dev):
        return pltpu.make_async_remote_copy(src_ref=buf.at[src_row], dst_ref=buf.at[src_row], send_sem=send_sem,
                                            recv_sem=recv_sem, device_id=(dev,), device_id_type=MESH)

    def exchange_start(buf, s_sem, r_sem):
        def go(i, _):
            row_copy(buf, me, s_sem.at[i], r_sem.at[me], lax.rem(me + i, N_DEV)).start()
            return 0
        lax.fori_loop(1, N_DEV, go, 0)

    def exchange_wait(buf, s_sem, r_sem):
        def go(i, _):
            peer = lax.rem(me + i, N_DEV)
            row_copy(buf, me, s_sem.at[i], r_sem.at[me], peer).wait_send()
            row_copy(buf, peer, s_sem.at[i], r_sem.at[peer], peer).wait_recv()
            return 0
        lax.fori_loop(1, N_DEV, go, 0)

    loads = [pltpu.make_async_copy(a, b, ls.at[i]) for i, (a, b) in enumerate((
        (x_hbm, x_ref), (msk_hbm, msk_ref), (w1_hbm, w1_ref), (w2_hbm, w2_ref), (h_hbm, h_ref), (lab_hbm, lab_ref)))]
    for cp in loads:
        cp.start()

    bar = pltpu.get_barrier_semaphore()

    def sig(i, _):
        pl.semaphore_signal(bar, inc=1, device_id=(lax.rem(me + i, N_DEV),), device_id_type=MESH)
        return 0
    lax.fori_loop(1, N_DEV, sig, 0)

    col = lax.broadcasted_iota(jnp.int32, (DIM, 1), 0)
    blk = (col * 43691) >> 19
    off = col - 12 * blk
    dev = (((blk >> 4) & 1) + 4 * ((blk >> 3) & 1) + ZB * ((blk >> 2) & 1) + ZA * ((blk >> 1) & 1) + 2 * (blk & 1))
    perm = (lax.broadcasted_iota(jnp.int32, (DIM, DIM), 1) == 12 * dev + off).astype(BF16)
    loads[0].wait()
    gx[0] = dot_nt(perm, x_ref[...]).astype(BF16)
    lane = lax.broadcasted_iota(jnp.int32, (1, 128), 1)
    row = jnp.zeros((1, 128), F32)
    loads[1].wait()
    for t in range(TASKS):
        row = row + jnp.where(lane == t, jnp.sum(msk_ref[t:t + 1, :].astype(F32), axis=1, keepdims=True), 0.0)
    cnts[me] = row

    pl.semaphore_wait(bar, N_DEV - 1)

    def chunk(k):
        return pl.ds(k * ROWS, ROWS)
    exchange_start(cnts, cs, cr)
    to_2 = [start(rcopy(gx.at[0, chunk(k)], gx.at[2, chunk(k)], to_za)) for k in range(CHUNKS)]
    to_1 = [start(rcopy(gx.at[0, chunk(k)], gx.at[1, chunk(k)], to_x)) for k in range(CHUNKS)]
    to_3 = [rcopy(gx.at[2, chunk(k)], gx.at[3, chunk(k)], to_x) for k in range(CHUNKS)]
    e_2 = rcopy(ge.at[0], ge.at[2], to_za)
    e_1 = rcopy(ge.at[0], ge.at[1], to_x)
    e_3 = rcopy(ge.at[2], ge.at[3], to_x)

    for cp in loads[2:]:
        cp.wait()
    hp_ref[...] = jnp.zeros_like(hp_ref)
    for t in range(TASKS):
        hp_ref[PAD * t:PAD * t + CLS, :] = h_ref[t]
    def fwd(i, _):
        cols = pl.ds(pl.multiple_of(i * 256, 256), 256)
        p = dot(x_ref[...], w1_ref[:, cols])
        a_own[:, cols] = (p * gelu_cdf(p)[2]).astype(BF16)
        return 0
    lax.fori_loop(0, HID // 256, fwd, 0)
    z = (x_ref[...].astype(F32) + dot(a_own[...], w2_ref[...])).astype(BF16)
    logits = dot_nt(hp_ref[...], z)
    cls = lax.broadcasted_iota(jnp.int32, (PAD, TOK), 0)
    valid = cls < CLS
    for t in range(TASKS):
        lg = jnp.where(valid, logits[PAD * t:PAD * (t + 1)], -jnp.inf)
        ex = jnp.exp(lg - jnp.max(lg, axis=0, keepdims=True))
        sm = ex / jnp.sum(ex, axis=0, keepdims=True)
        hot = (lab_ref[t:t + 1, :] == cls).astype(F32)
        ge[0, t] = jnp.where(valid, msk_ref[t:t + 1, :].astype(F32) * (sm - hot), 0.0).astype(BF16)
    start(e_2)
    start(e_1)

    seg = (col * 43691) >> 21
    src = 48 * (((seg >> 2) & 1) + ZB * ((seg >> 1) & 1) + 4 * (seg & 1) + ZA * za + 2 * x) + (col - 48 * seg)
    sel = (lax.broadcasted_iota(jnp.int32, (DIM, HID), 1) == src).astype(BF16)
    w1_rows = dot_nt(sel, w1_ref[...]).astype(BF16)
    w1s[...] = dot_nt(w1_rows, perm).astype(BF16)
    for k in range(8):
        dv = ((k >> 2) & 1) + ZB * ((k >> 1) & 1) + 4 * (k & 1) + ZA * za + 2 * x
        w2s[48 * k:48 * (k + 1), :] = w2_ref[pl.ds(pl.multiple_of(48 * dv, 16), 48), :]
    for t in range(TASKS):
        ht[t] = jnp.transpose(hp_ref[PAD * t:PAD * (t + 1), :].astype(F32)).astype(BF16)

    def acts(s):
        for r in range(3):
            rows = slice(128 * r, 128 * (r + 1))
            p = dot(w1s[rows, :], gx[s])
            sq, t, cdf = gelu_cdf(p)
            a_t[rows, :] = (p * cdf).astype(BF16)
            gp[rows, :] = cdf + (0.5 * GELU_C) * p * (1.0 - t * t) * (1.0 + (3.0 * GELU_A) * sq)

    def grads(s, t, first):
        dz[...] = dot(ht[t], ge[s, t]).astype(BF16)
        for r in range(3):
            rows = slice(128 * r, 128 * (r + 1))
            qt[rows, :] = (dot(w2s[rows, :], dz[...]) * gp[rows, :]).astype(BF16)
        sc = inv[t]
        d1 = (dot_nt(gx[s], qt[...]) * sc).astype(BF16).astype(F32)
        acc1[t] = d1 if first else acc1[t] + d1
        d2 = (dot_nt(a_t[...], dz[...]) * sc).astype(BF16).astype(F32)
        acc2[t] = d2 if first else acc2[t] + d2

    acts(0)
    exchange_wait(cnts, cs, cr)
    total = jnp.sum(cnts[...], axis=0)
    recip = 1.0 / jnp.maximum(total, 1.0)
    for t in range(TASKS):
        inv[t] = jnp.broadcast_to(recip[:, t:t + 1], (1, DIM))
    for t in range(TASKS):
        grads(0, t, True)
    to_2[0].wait_recv()
    start(to_3[0])
    for cp in to_1:
        cp.wait_recv()
    acts(1)
    to_2[1].wait_recv()
    start(to_3[1])
    e_1.wait_recv()
    for t in range(TASKS):
        grads(1, t, False)
    to_2[2].wait_recv()
    start(to_3[2])
    to_2[3].wait_recv()
    start(to_3[3])
    e_2.wait_recv()
    start(e_3)
    acts(2)
    for t in range(TASKS):
        grads(2, t, False)
    for cp in to_3:
        cp.wait_recv()
    acts(3)
    e_3.wait_recv()

    def rows_of(base, n):
        return pl.ds(pl.multiple_of(base, 48), n)
    c1, c2 = [], []
    for t in range(TASKS):
        grads(3, t, False)
        c1.append(start(rcopy(acc1.at[t, rows_of(192 * (1 - c), 192)], rc1.at[t], to_c)))
        c2.append(start(rcopy(acc2.at[t, rows_of(192 * (1 - c), 192)], rc2.at[t], to_c)))
    b0 = 192 * c
    h1, h2 = [], []
    for t in range(TASKS):
        c1[t].wait_recv()
        mine = rows_of(b0, 192)
        acc1[t, mine] = acc1[t, mine] + rc1[t]
        h1.append(start(rcopy(acc1.at[t, rows_of(b0 + 96 * (1 - y), 96)], ra1.at[t], to_y)))
        c2[t].wait_recv()
        acc2[t, mine] = acc2[t, mine] + rc2[t]
        h2.append(start(rcopy(acc2.at[t, rows_of(b0 + 96 * (1 - zb), 96)], ra2.at[t], to_zb)))
    q1, q2 = [], []
    for t in range(TASKS):
        h1[t].wait_recv()
        mine = rows_of(b0 + 96 * y, 96)
        acc1[t, mine] = acc1[t, mine] + ra1[t]
        q1.append(start(rcopy(acc1.at[t, rows_of(b0 + 96 * y + 48 * (1 - zb), 48)], rb1.at[t], to_zb)))
        h2[t].wait_recv()
        mine = rows_of(b0 + 96 * zb, 96)
        acc2[t, mine] = acc2[t, mine] + ra2[t]
        q2.append(start(rcopy(acc2.at[t, rows_of(b0 + 96 * zb + 48 * (1 - y), 48)], rb2.at[t], to_y)))
    own = 2 * za + x
    zero4 = jnp.zeros((4, DIM), F32)
    for t in range(TASKS):
        q1[t].wait_recv()
        g = acc1[t, rows_of(b0 + 96 * y + 48 * zb, 48)] + rb1[t]
        g1s[t] = g
        for k in range(4):
            sb[k, t] = jnp.concatenate([g[12 * k:12 * (k + 1)], zero4], axis=0)
        q2[t].wait_recv()
        g2s[t] = acc2[t, rows_of(b0 + 96 * zb + 48 * y, 48)] + rb2[t]

    row = jnp.zeros((1, 128), F32)
    pairs = [(0, 0), (0, 1), (0, 2), (1, 1), (1, 2), (2, 2)]
    for i, (t, s) in enumerate(pairs):
        part = jnp.sum(g1s[t] * g1s[s] + g2s[t] * g2s[s], axis=0, keepdims=True)
        row = row + jnp.where(lane == i, jnp.sum(part, axis=1, keepdims=True), 0.0)
    grams[me] = row
    exchange_start(grams, gs, gr)
    fx, fz = 1 - 2 * x, 2 * (1 - 2 * za)
    back = []
    for dk, to in ((fx, to_x), (fz, to_za), (fx + fz, to_x + to_za - me)):
        back.append(start(rcopy(sb.at[own + dk], rb.at[own], to)))
    rb[own] = sb[own]
    for t in range(TASKS):
        for k in range(3):
            o2_ref[t, pl.ds(k, 48, stride=3), :] = g2s[t, :, 128 * k:128 * (k + 1)]
    for cp in back:
        cp.wait_recv()
    for t in range(TASKS):
        parts = []
        for b in range(32):
            bza, bzb, by, bx, bc = b >> 4, (b >> 3) & 1, (b >> 2) & 1, (b >> 1) & 1, b & 1
            at = 192 * bc + 96 * bzb + 48 * by
            parts.append(rb[2 * bza + bx, t, :, at:at + 48])
        full = jnp.concatenate(parts, axis=1)
        for k in range(12):
            o1_ref[t, pl.ds(k, 12, stride=12), :] = full[:12, 128 * k:128 * (k + 1)]
    exchange_wait(grams, gs, gr)
    m = jnp.sum(grams[...], axis=0)
    ent = [jnp.broadcast_to(m[:, i:i + 1], (8, 128)) for i in range(6)]
    neg = -TASKS / (ent[0] + ent[3] + ent[5])
    gram = {}
    for i, (t, s) in enumerate(pairs):
        gram[t, s] = gram[s, t] = ent[i] * neg
    w = [jnp.full((8, 128), 1.0 / TASKS, F32)] * TASKS
    for _ in range(SOLVER_STEPS):
        up = [w[t] * jnp.exp(gram[t, 0] * w[0] + gram[t, 1] * w[1] + gram[t, 2] * w[2]) for t in range(TASKS)]
        norm = 1.0 / (up[0] + up[1] + up[2])
        w = [u * norm for u in up]
    al_ref[...] = jnp.where(lane == 0, w[0][:1], jnp.where(lane == 1, w[1][:1], w[2][:1]))[:, :TASKS]
    for cp in pending:
        cp.wait_send()


def solution(mesh):
    def step(tokens, w_in, w_out, heads, lab, msk):
        vm = pl.BlockSpec(memory_space=pltpu.VMEM)
        dma = pltpu.SemaphoreType.DMA
        alpha, g1, g2 = pl.pallas_call(
            kernel,
            name="step",
            out_shape=(jax.ShapeDtypeStruct((1, TASKS), F32), jax.ShapeDtypeStruct((TASKS, 144, 128), F32),
                       jax.ShapeDtypeStruct((TASKS, 144, 128), F32)),
            in_specs=[pl.BlockSpec(memory_space=pl.ANY)] * 6,
            out_specs=(vm, vm, vm),
            scratch_shapes=[
                pltpu.VMEM((TOK, DIM), BF16), pltpu.VMEM((DIM, HID), BF16), pltpu.VMEM((HID, DIM), BF16),
                pltpu.VMEM((TASKS, CLS, DIM), BF16), pltpu.VMEM((TASKS, TOK), jnp.int32),
                pltpu.VMEM((TASKS, TOK), jnp.int32), pltpu.VMEM((TASKS * PAD, DIM), BF16),
                pltpu.VMEM((N_DEV, 1, 128), F32), pltpu.VMEM((N_DEV, 1, 128), F32),
                pltpu.VMEM((4, DIM, TOK), BF16), pltpu.VMEM((4, TASKS, PAD, TOK), BF16),
                pltpu.VMEM((TASKS, DIM, PAD), BF16), pltpu.VMEM((DIM, DIM), BF16), pltpu.VMEM((DIM, DIM), BF16),
                pltpu.VMEM((TOK, HID), BF16), pltpu.VMEM((DIM, TOK), BF16), pltpu.VMEM((DIM, TOK), F32),
                pltpu.VMEM((DIM, TOK), BF16), pltpu.VMEM((DIM, TOK), BF16), pltpu.VMEM((TASKS, 1, DIM), F32),
                pltpu.VMEM((TASKS, DIM, DIM), F32), pltpu.VMEM((TASKS, DIM, DIM), F32),
                pltpu.VMEM((TASKS, 192, DIM), F32), pltpu.VMEM((TASKS, 192, DIM), F32),
                pltpu.VMEM((TASKS, 96, DIM), F32), pltpu.VMEM((TASKS, 96, DIM), F32),
                pltpu.VMEM((TASKS, 48, DIM), F32), pltpu.VMEM((TASKS, 48, DIM), F32),
                pltpu.VMEM((TASKS, 48, DIM), F32), pltpu.VMEM((TASKS, 48, DIM), F32),
                pltpu.VMEM((4, TASKS, 16, DIM), F32), pltpu.VMEM((4, TASKS, 16, DIM), F32),
                dma((N_SEM,)), dma((N_SEM,)), dma((N_DEV,)), dma((N_DEV,)), dma((N_DEV,)), dma((N_DEV,)),
                dma((6,)),
            ],
            compiler_params=pltpu.CompilerParams(collective_id=0, has_side_effects=True, vmem_limit_bytes=56 * 2**20),
        )(tokens, w_in, w_out, heads.transpose(0, 2, 1), lab, msk)
        alpha = alpha.reshape(TASKS)
        w = alpha[:, None, None]
        return alpha, (w * g1).sum(axis=0).reshape(-1), (w * g2).sum(axis=0).reshape(-1)

    return jax.shard_map(step, mesh=mesh, in_specs=(P("data", None), P(), P(), P(), P(None, "data"), P(None, "data")),
                         out_specs=(P(), P("data"), P("data")), check_vma=False)
```

```python
import jax
import jax.numpy as jnp
from jax import lax
from jax.experimental import pallas as pl
from jax.experimental.pallas import tpu as pltpu
from jax.sharding import PartitionSpec as P

MESH = pl.DeviceIdType.MESH
SOLVER_STEPS = 20
N_DEV = 32
TOK, DIM, HID, TASKS, CLS, PAD = 512, 384, 1536, 3, 13, 16
HALF = TOK // 2
GELU_C = 0.7978845608028654
GELU_A = 0.044715
N_SEM = 69
OWN, FROM_X, FROM_Z, FROM_XZ, FROM_Y, FROM_YZ = range(6)

F32, BF16 = jnp.float32, jnp.bfloat16


def dot(a, b):
    return jnp.dot(a, b, preferred_element_type=F32)


def dot_nt(a, b):
    return lax.dot_general(a, b, (((1,), (1,)), ((), ())), preferred_element_type=F32)


def gelu_cdf(p):
    sq = p * p
    t = jnp.tanh(GELU_C * (p + GELU_A * (sq * p)))
    return sq, t, 0.5 * (1.0 + t)


def kernel(x_hbm, w1_hbm, w2_hbm, h_hbm, lab_hbm, msk_hbm, al_ref, o1_ref, o2_ref,
           x_ref, w1_ref, w2_ref, h_ref, lab_ref, msk_ref, hp_ref, cnts, grams,
           gx, ge, ht, w1a, w1b, w2a, a_own, at, gp, dz, dzx, qt, inv, acc1, acc2,
           rc1, rc2, ra1, ra2, rb1, rb2, g1s, g2s, sb, rb,
           ss, rs, ls):
    me = lax.axis_index("data")
    c = lax.rem(me, 2)
    x = lax.rem(me // 2, 2)
    y = lax.rem(me // 4, 2)
    zl = lax.rem(me // 8, 2)
    zh = lax.rem(me // 16, 2)
    to_c = me + (1 - 2 * c)
    to_x = me + 2 * (1 - 2 * x)
    to_y = me + 4 * (1 - 2 * y)
    to_zl = me + 8 * (1 - 2 * zl)
    to_zh = me + 16 * (1 - 2 * zh)

    used = []

    def rcopy(src, dst, dev, group):
        i = len(used)
        used.append(i)
        return pltpu.make_async_remote_copy(src_ref=src, dst_ref=dst, send_sem=ss.at[group], recv_sem=rs.at[i],
                                            device_id=(dev,), device_id_type=MESH)

    def start(cp):
        cp.start()
        return cp

    def wait_bytes(ref, sem):
        pltpu.make_async_copy(ref, ref, sem).wait()

    def row_copy(buf, src_row, send_sem, recv_sem, dev):
        return pltpu.make_async_remote_copy(src_ref=buf.at[src_row], dst_ref=buf.at[src_row], send_sem=send_sem,
                                            recv_sem=recv_sem, device_id=(dev,), device_id_type=MESH)

    def exchange_start(buf, s_sem, r_sem):
        def go(i, _):
            row_copy(buf, me, s_sem, r_sem, lax.rem(me + i, N_DEV)).start()
            return 0
        lax.fori_loop(1, N_DEV, go, 0)

    def exchange_wait(buf, sem):
        wait_bytes(buf.at[pl.ds(0, N_DEV - 1)], sem)

    loads = [pltpu.make_async_copy(a, b, ls.at[i]) for i, (a, b) in enumerate((
        (x_hbm, x_ref), (msk_hbm, msk_ref), (w1_hbm, w1_ref), (w2_hbm, w2_ref), (h_hbm, h_ref), (lab_hbm, lab_ref)))]
    for cp in loads:
        cp.start()

    bar = pltpu.get_barrier_semaphore()

    def sig(i, _):
        pl.semaphore_signal(bar, inc=1, device_id=(lax.rem(me + i, N_DEV),), device_id_type=MESH)
        return 0
    lax.fori_loop(1, N_DEV, sig, 0)

    col = lax.broadcasted_iota(jnp.int32, (DIM, 1), 0)
    blk = (col * 43691) >> 19
    dev = ((blk >> 3) & 1) + 4 * ((blk >> 2) & 1) + 8 * ((blk >> 1) & 1) + 16 * ((blk >> 4) & 1) + 2 * (blk & 1)
    perm = (lax.broadcasted_iota(jnp.int32, (DIM, DIM), 1) == 12 * dev + (col - 12 * blk)).astype(BF16)
    loads[0].wait()
    for h in range(2):
        gx[OWN, h] = dot_nt(perm, x_ref[HALF * h:HALF * (h + 1), :]).astype(BF16)
    lane = lax.broadcasted_iota(jnp.int32, (1, 128), 1)
    row = jnp.zeros((1, 128), F32)
    loads[1].wait()
    for t in range(TASKS):
        row = row + jnp.where(lane == t, jnp.sum(msk_ref[t:t + 1, :].astype(F32), axis=1, keepdims=True), 0.0)
    cnts[me] = row

    pl.semaphore_wait(bar, N_DEV - 1)

    def piece(slot, h, r0=0, n=DIM):
        return gx.at[slot, h, pl.ds(r0, n)]
    cuts = ((0, 0, 192), (0, 192, 192), (1, 0, 192), (1, 192, 128), (1, 320, 64))
    z_x = [rcopy(piece(OWN, *k), piece(FROM_Z, *k), to_zh, 0) for k in cuts]
    x_x = [rcopy(piece(OWN, h), piece(FROM_X, h), to_x, 0) for h in range(2)]
    y_x = [rcopy(piece(OWN, h), piece(FROM_Y, h), to_y, 0) for h in range(2)]
    xz_x = [rcopy(piece(FROM_Z, *k), piece(FROM_XZ, *k), to_x, 0) for k in cuts]
    yz_x = [rcopy(piece(FROM_Z, *k), piece(FROM_YZ, *k), to_y, 0) for k in cuts]
    z_e = rcopy(ge.at[OWN], ge.at[FROM_Z], to_zh, 1)
    x_e = rcopy(ge.at[OWN], ge.at[FROM_X], to_x, 1)
    y_e = rcopy(ge.at[OWN], ge.at[FROM_Y], to_y, 1)
    xz_e = rcopy(ge.at[FROM_Z], ge.at[FROM_XZ], to_x, 1)
    yz_e = rcopy(ge.at[FROM_Z], ge.at[FROM_YZ], to_y, 1)

    def forward(got, a, b):
        got.wait_recv()
        start(a)
        start(b)

    exchange_start(cnts, ls.at[6], ls.at[7])
    start(z_x[0])
    start(x_x[0])
    start(y_x[0])

    for cp in loads[2:]:
        cp.wait()
    hp_ref[...] = jnp.zeros_like(hp_ref)
    for t in range(TASKS):
        hp_ref[PAD * t:PAD * t + CLS, :] = h_ref[t]

    def fwd(i, _):
        cols = pl.ds(pl.multiple_of(i * 256, 256), 256)
        p = dot(x_ref[...], w1_ref[:, cols])
        a_own[:, cols] = (p * gelu_cdf(p)[2]).astype(BF16)
        return 0
    lax.fori_loop(0, HID // 256, fwd, 0)
    start(z_x[1])
    z = (x_ref[...].astype(F32) + dot(a_own[...], w2_ref[...])).astype(BF16)
    logits = dot_nt(hp_ref[...], z)
    cls = lax.broadcasted_iota(jnp.int32, (PAD, TOK), 0)
    valid = cls < CLS
    for t in range(TASKS):
        lg = jnp.where(valid, logits[PAD * t:PAD * (t + 1)], -jnp.inf)
        ex = jnp.exp(lg - jnp.max(lg, axis=0, keepdims=True))
        sm = ex / jnp.sum(ex, axis=0, keepdims=True)
        hot = (lab_ref[t:t + 1, :] == cls).astype(F32)
        ge[OWN, t] = jnp.where(valid, msk_ref[t:t + 1, :].astype(F32) * (sm - hot), 0.0).astype(BF16)
    start(z_e)
    start(x_e)
    start(y_e)
    start(x_x[1])
    start(y_x[1])

    hid_iota = lax.broadcasted_iota(jnp.int32, (DIM, HID), 1)
    seg = (col * 43691) >> 21
    src_a = 48 * ((seg >> 2) + 8 * ((seg >> 1) & 1) + 4 * (seg & 1) + 16 * zh + 2 * x) + (col - 48 * seg)
    seg = (col * 43691) >> 20
    src_b = (48 * (((seg >> 2) & 1) + 2 * ((seg >> 1) & 1) + 8 * (seg & 1) + 16 * zh + 4 * y)
             + 24 * (seg >> 3) + (col - 24 * seg))
    for src, dst in ((src_a, w1a), (src_b, w1b)):
        sel = (hid_iota == src).astype(BF16)
        dst[...] = dot_nt(dot_nt(sel, w1_ref[...]).astype(BF16), perm).astype(BF16)
    for k in range(8):
        dv = (k >> 2) + 8 * ((k >> 1) & 1) + 4 * (k & 1) + 16 * zh + 2 * x
        w2a[48 * k:48 * (k + 1), :] = w2_ref[pl.ds(pl.multiple_of(48 * dv, 16), 48), :]
    for t in range(TASKS):
        ht[t] = jnp.transpose(hp_ref[PAD * t:PAD * (t + 1), :].astype(F32)).astype(BF16)

    strips = [slice(128 * r, 128 * (r + 1)) for r in range(3)]

    def slope(s, h):
        for rows in strips:
            p = dot(w1a[rows, :], gx[s, h])
            sq, t, cdf = gelu_cdf(p)
            gp[rows, :] = cdf + (0.5 * GELU_C) * p * (1.0 - t * t) * (1.0 + (3.0 * GELU_A) * sq)

    def act(s, h, k):
        for rows in strips:
            p = dot(w1b[rows, :], gx[s, h])
            at[k, h, rows, :] = (p * gelu_cdf(p)[2]).astype(BF16)

    def dz_of(s, h, t, ref):
        ref[...] = dot(ht[t], ge[s, t, :, HALF * h:HALF * (h + 1)]).astype(BF16)

    def q_of(h, t, k, ref):
        for rows in strips:
            qt[k, t, h, rows, :] = (dot(w2a[rows, :], ref[...]) * gp[rows, :]).astype(BF16)

    def prep_a(s, h, k):
        slope(s, h)
        for t in range(TASKS):
            dz_of(s, h, t, dzx)
            q_of(h, t, k, dzx)

    def prep_b(s, h, k):
        act(s, h, k)
        for t in range(TASKS):
            dz_of(s, h, t, dz.at[k, t, h])

    def prep(s, h):
        slope(s, h)
        act(s, h, 0)
        for t in range(TASKS):
            dz_of(s, h, t, dz.at[0, t, h])
            q_of(h, t, 0, dz.at[0, t, h])

    def add_a(s, t, k, first=False):
        d = dot_nt(gx[s, 0], qt[k, t, 0]) + dot_nt(gx[s, 1], qt[k, t, 1])
        d = (d * inv[t]).astype(BF16).astype(F32)
        acc1[t] = d if first else acc1[t] + d

    def add_b(t, k, first=False):
        d = dot_nt(at[k, 0], dz[k, t, 0]) + dot_nt(at[k, 1], dz[k, t, 1])
        d = (d * inv[t]).astype(BF16).astype(F32)
        acc2[t] = d if first else acc2[t] + d

    prep(OWN, 0)
    prep(OWN, 1)
    start(z_x[2])
    exchange_wait(cnts, ls.at[7])
    total = jnp.sum(cnts[...], axis=0)
    recip = 1.0 / jnp.maximum(total, 1.0)
    for t in range(TASKS):
        inv[t] = jnp.broadcast_to(recip[:, t:t + 1], (1, DIM))
    for t in range(TASKS):
        add_a(OWN, t, 0, True)
        add_b(t, 0, True)
    start(z_x[3])
    for cp in (x_e, x_x[0], x_x[1]):
        cp.wait_recv()
    prep_a(FROM_X, 0, 0)
    start(z_x[4])
    forward(z_x[0], xz_x[0], yz_x[0])
    prep_a(FROM_X, 1, 0)
    for t in range(TASKS):
        add_a(FROM_X, t, 0)
    for cp in (y_e, y_x[0], y_x[1]):
        cp.wait_recv()
    prep_b(FROM_Y, 0, 0)
    prep_b(FROM_Y, 1, 0)
    for t in range(TASKS):
        add_b(t, 0)
    forward(z_e, xz_e, yz_e)
    forward(z_x[1], xz_x[1], yz_x[1])
    prep(FROM_Z, 0)
    forward(z_x[2], xz_x[2], yz_x[2])
    forward(z_x[3], xz_x[3], yz_x[3])
    forward(z_x[4], xz_x[4], yz_x[4])
    for cp in (xz_e, xz_x[0], xz_x[1]):
        cp.wait_recv()
    prep_a(FROM_XZ, 0, 1)
    for cp in (yz_e, yz_x[0], yz_x[1]):
        cp.wait_recv()
    prep_b(FROM_YZ, 0, 1)
    prep(FROM_Z, 1)
    for cp in xz_x[2:]:
        cp.wait_recv()
    for cp in yz_x[2:]:
        cp.wait_recv()

    def rows(base, n):
        return pl.ds(pl.multiple_of(base, 8), n)
    bits1, bits2 = (c, y, zl), (c, x, zl)
    dest1, dest2 = (to_c, to_y, to_zl), (to_c, to_x, to_zl)
    size = (96, 48, 24)

    def base(bits, u, stage):
        at0 = 192 * u
        for i in range(stage):
            at0 = at0 + size[i] * bits[i]
        return at0

    def send(acc, recv, bits, dest, t, u, stage, group):
        at0 = base(bits, u, stage) + size[stage] * (1 - bits[stage])
        return start(rcopy(acc.at[t, rows(at0, size[stage])], recv.at[t, u], dest[stage], group))

    part1 = (acc1, (rc1, ra1, rb1), bits1, dest1)
    part2 = (acc2, (rc2, ra2, rb2), bits2, dest2)
    order = [(t, u) for t in range(TASKS) for u in range(2)]
    cps = {}

    def go(part, i, t, u, stage):
        acc, recv, bits, dest = part
        cps[i, t, u, stage] = send(acc, recv[stage], bits, dest, t, u, stage, 2 * stage + i + 1)

    def merge(part, t, u, stage):
        acc, recv, bits, _ = part
        mine = rows(base(bits, u, stage) + size[stage] * bits[stage], size[stage])
        v = acc[t, mine] + recv[stage][t, u]
        acc[t, mine] = v
        return v

    def add(part, i, t, u, stage):
        cps[i, t, u, stage].wait_recv()
        return merge(part, t, u, stage)

    own = 2 * zh + x
    fx, fz = 1 - 2 * x, 2 * (1 - 2 * zh)
    back = []

    def send_back(t):
        for dk, to in ((fz, to_zh), (fx + fz, to_x + to_zh - me), (fx, to_x)):
            back.append(start(rcopy(sb.at[own + dk, t], rb.at[own, t], to, 8)))

    def finish(t, u):
        g = add(part1, 1, t, u, 2)
        g1s[t, 24 * u:24 * (u + 1)] = g
        for k in range(2):
            sb[2 * u + k, t] = g[12 * k:12 * (k + 1)]
        if u == 1 and t < TASKS - 1:
            send_back(t)
        g2s[t, 24 * u:24 * (u + 1)] = add(part2, 2, t, u, 2)

    both = ((1, part1), (2, part2))

    def first_hop(n):
        for i, part in both:
            add(part, i, *order[n], 0)
            go(part, i, *order[n], 1)

    slope(FROM_XZ, 1)
    act(FROM_YZ, 1, 1)
    for t in range(TASKS):
        dz_of(FROM_XZ, 1, t, dzx)
        q_of(1, t, 1, dzx)
        add_a(FROM_Z, t, 0)
        add_a(FROM_XZ, t, 1)
        for u in range(2):
            go(part1, 1, t, u, 0)
        dz_of(FROM_YZ, 1, t, dz.at[1, t, 1])
        add_b(t, 0)
        add_b(t, 1)
        for u in range(2):
            go(part2, 2, t, u, 0)
        if t == 1:
            first_hop(0)
            first_hop(1)
    first_hop(2)
    for n in range(6):
        if n + 3 < 6:
            for i, part in both:
                add(part, i, *order[n + 3], 0)
        for i, part in both:
            cps[i, *order[n], 1].wait_recv()
            if n + 3 < 6:
                go(part, i, *order[n + 3], 1)
            merge(part, *order[n], 1)
            go(part, i, *order[n], 2)
        if n >= 2:
            finish(*order[n - 2])
    finish(*order[4])
    finish(*order[5])

    row = jnp.zeros((1, 128), F32)
    pairs = [(0, 0), (0, 1), (0, 2), (1, 1), (1, 2), (2, 2)]
    for i, (t, s) in enumerate(pairs):
        part = jnp.sum(g1s[t] * g1s[s] + g2s[t] * g2s[s], axis=0, keepdims=True)
        row = row + jnp.where(lane == i, jnp.sum(part, axis=1, keepdims=True), 0.0)
    grams[me] = row
    exchange_start(grams, ls.at[8], ls.at[9])
    send_back(TASKS - 1)
    rb[own] = sb[own]
    for t in range(TASKS):
        for k in range(3):
            o2_ref[t, pl.ds(k, 48, stride=3), :] = g2s[t, :, 128 * k:128 * (k + 1)]
    for cp in back:
        cp.wait_recv()
    for t in range(TASKS):
        parts = []
        for b in range(32):
            bzh, bzl, by, bx, bc = b >> 4, (b >> 3) & 1, (b >> 2) & 1, (b >> 1) & 1, b & 1
            at0 = 192 * bc + 96 * bzl + 48 * by
            parts.append(rb[2 * bzh + bx, t, :, at0:at0 + 48])
        full = jnp.concatenate(parts, axis=1)
        for k in range(12):
            o1_ref[t, pl.ds(k, 12, stride=12), :] = full[:, 128 * k:128 * (k + 1)]
    exchange_wait(grams, ls.at[9])
    m = jnp.sum(grams[...], axis=0)
    ent = [jnp.broadcast_to(m[:, i:i + 1], (8, 128)) for i in range(6)]
    neg = -TASKS / (ent[0] + ent[3] + ent[5])
    gram = {}
    for i, (t, s) in enumerate(pairs):
        gram[t, s] = gram[s, t] = ent[i] * neg
    w = [jnp.full((8, 128), 1.0 / TASKS, F32)] * TASKS
    for _ in range(SOLVER_STEPS):
        up = [w[t] * jnp.exp(gram[t, 0] * w[0] + gram[t, 1] * w[1] + gram[t, 2] * w[2]) for t in range(TASKS)]
        norm = 1.0 / (up[0] + up[1] + up[2])
        w = [v * norm for v in up]
    al_ref[...] = jnp.where(lane == 0, w[0][:1], jnp.where(lane == 1, w[1][:1], w[2][:1]))[:, :TASKS]
    exchange_wait(cnts, ls.at[6])
    exchange_wait(grams, ls.at[8])
    for i, ref in enumerate((gx.at[pl.ds(0, 5)], ge.at[pl.ds(0, 5)], rc1, rc2, ra1, ra2, rb1, rb2, rb.at[pl.ds(0, 3)])):
        wait_bytes(ref, ss.at[i])


def solution(mesh):
    def step(tokens, w_in, w_out, heads, lab, msk):
        vm = pl.BlockSpec(memory_space=pltpu.VMEM)
        dma = pltpu.SemaphoreType.DMA
        v = pltpu.VMEM
        alpha, g1, g2 = pl.pallas_call(
            kernel,
            name="step",
            out_shape=(jax.ShapeDtypeStruct((1, TASKS), F32), jax.ShapeDtypeStruct((TASKS, 144, 128), F32),
                       jax.ShapeDtypeStruct((TASKS, 144, 128), F32)),
            in_specs=[pl.BlockSpec(memory_space=pltpu.HBM)] * 6,
            out_specs=(vm, vm, vm),
            scratch_shapes=[
                v((TOK, DIM), BF16), v((DIM, HID), BF16), v((HID, DIM), BF16),
                v((TASKS, CLS, DIM), BF16), v((TASKS, TOK), jnp.int32),
                v((TASKS, TOK), jnp.int32), v((TASKS * PAD, DIM), BF16),
                v((N_DEV, 1, 128), F32), v((N_DEV, 1, 128), F32),
                v((6, 2, DIM, HALF), BF16), v((6, TASKS, PAD, TOK), BF16),
                v((TASKS, DIM, PAD), BF16), v((DIM, DIM), BF16), v((DIM, DIM), BF16), v((DIM, DIM), BF16),
                v((TOK, HID), BF16), v((2, 2, DIM, HALF), BF16), v((DIM, HALF), F32),
                v((2, TASKS, 2, DIM, HALF), BF16), v((DIM, HALF), BF16), v((2, TASKS, 2, DIM, HALF), BF16),
                v((TASKS, 1, DIM), F32),
                v((TASKS, DIM, DIM), F32), v((TASKS, DIM, DIM), F32),
                v((TASKS, 2, 96, DIM), F32), v((TASKS, 2, 96, DIM), F32),
                v((TASKS, 2, 48, DIM), F32), v((TASKS, 2, 48, DIM), F32),
                v((TASKS, 2, 24, DIM), F32), v((TASKS, 2, 24, DIM), F32),
                v((TASKS, 48, DIM), F32), v((TASKS, 48, DIM), F32),
                v((4, TASKS, 12, DIM), F32), v((4, TASKS, 12, DIM), F32),
                dma((9,)), dma((N_SEM,)), dma((10,)),
            ],
            compiler_params=pltpu.CompilerParams(collective_id=0, has_side_effects=True, vmem_limit_bytes=28 * 2**20),
        )(*[pltpu.with_memory_space_constraint(a, pltpu.HBM)
            for a in (tokens, w_in, w_out, heads.transpose(0, 2, 1), lab, msk)])
        alpha = alpha.reshape(TASKS)
        w = alpha[:, None, None]
        return alpha, (w * g1).sum(axis=0).reshape(-1), (w * g2).sum(axis=0).reshape(-1)

    return jax.shard_map(step, mesh=mesh, in_specs=(P("data", None), P(), P(), P(), P(None, "data"), P(None, "data")),
                         out_specs=(P(), P("data"), P("data")), check_vma=False)
```

```python
import jax
import jax.numpy as jnp
from jax import lax
from jax.experimental import pallas as pl
from jax.experimental.pallas import tpu as pltpu
from jax.sharding import PartitionSpec as P

MESH = pl.DeviceIdType.MESH
SOLVER_STEPS = 20
N_DEV = 32
TOK, DIM, HID, TASKS, CLS, PAD = 512, 384, 1536, 3, 13, 16
HALF = TOK // 2
GELU_C = 0.7978845608028654
GELU_A = 0.044715
N_SEM = 68
OWN, FROM_X, FROM_Z, FROM_XZ, FROM_Y, FROM_YZ = range(6)

F32, BF16 = jnp.float32, jnp.bfloat16


def dot(a, b):
    return jnp.dot(a, b, preferred_element_type=F32)


def dot_nt(a, b):
    return lax.dot_general(a, b, (((1,), (1,)), ((), ())), preferred_element_type=F32)


def gelu_cdf(p):
    sq = p * p
    t = jnp.tanh(GELU_C * (p + GELU_A * (sq * p)))
    return sq, t, 0.5 * (1.0 + t)


def kernel(x_hbm, w1_hbm, w2_hbm, h_hbm, lab_hbm, msk_hbm, al_ref, o1_ref, o2_ref,
           x_ref, w1_ref, w2_ref, h_ref, lab_ref, msk_ref, hp_ref, cnts, grams,
           gx, ge, ht, w1a, w1b, w2a, a_own, at, gp, dz, dzx, qt, inv, acc1, acc2,
           rc1, rc2, ra1, ra2, rb1, rb2, g1s, g2s, sb, rb,
           ss, rs, ls):
    me = lax.axis_index("data")
    c = lax.rem(me, 2)
    x = lax.rem(me // 2, 2)
    y = lax.rem(me // 4, 2)
    zl = lax.rem(me // 8, 2)
    zh = lax.rem(me // 16, 2)
    to_c = me + (1 - 2 * c)
    to_x = me + 2 * (1 - 2 * x)
    to_y = me + 4 * (1 - 2 * y)
    to_zl = me + 8 * (1 - 2 * zl)
    to_zh = me + 16 * (1 - 2 * zh) + 8 * (1 - 2 * zl)
    e = lax.rem(zh + zl, 2)

    used = []

    def rcopy(src, dst, dev, group):
        i = len(used)
        used.append(i)
        return pltpu.make_async_remote_copy(src_ref=src, dst_ref=dst, send_sem=ss.at[group], recv_sem=rs.at[i],
                                            device_id=(dev,), device_id_type=MESH)

    def start(cp):
        cp.start()
        return cp

    def wait_bytes(ref, sem):
        pltpu.make_async_copy(ref, ref, sem).wait()

    def row_copy(buf, src_row, send_sem, recv_sem, dev):
        return pltpu.make_async_remote_copy(src_ref=buf.at[src_row], dst_ref=buf.at[src_row], send_sem=send_sem,
                                            recv_sem=recv_sem, device_id=(dev,), device_id_type=MESH)

    def exchange_start(buf, s_sem, r_sem):
        def go(i, _):
            row_copy(buf, me, s_sem, r_sem, lax.rem(me + i, N_DEV)).start()
            return 0
        lax.fori_loop(1, N_DEV, go, 0)

    def exchange_wait(buf, sem):
        wait_bytes(buf.at[pl.ds(0, N_DEV - 1)], sem)

    loads = [pltpu.make_async_copy(a, b, ls.at[i]) for i, (a, b) in enumerate((
        (x_hbm, x_ref), (msk_hbm, msk_ref), (w1_hbm, w1_ref), (w2_hbm, w2_ref), (h_hbm, h_ref), (lab_hbm, lab_ref)))]
    for cp in loads:
        cp.start()

    bar = pltpu.get_barrier_semaphore()

    def sig(i, _):
        pl.semaphore_signal(bar, inc=1, device_id=(lax.rem(me + i, N_DEV),), device_id_type=MESH)
        return 0
    lax.fori_loop(1, N_DEV, sig, 0)

    col = lax.broadcasted_iota(jnp.int32, (DIM, 1), 0)
    blk = (col * 43691) >> 19
    dev = (((blk >> 3) & 1) + 4 * ((blk >> 2) & 1) + 8 * (((blk >> 1) ^ (blk >> 4)) & 1) + 16 * ((blk >> 4) & 1)
           + 2 * (blk & 1))
    perm = (lax.broadcasted_iota(jnp.int32, (DIM, DIM), 1) == 12 * dev + (col - 12 * blk)).astype(BF16)
    loads[0].wait()
    for h in range(2):
        gx[OWN, h] = dot_nt(perm, x_ref[HALF * h:HALF * (h + 1), :]).astype(BF16)
    lane = lax.broadcasted_iota(jnp.int32, (1, 128), 1)
    row = jnp.zeros((1, 128), F32)
    loads[1].wait()
    for t in range(TASKS):
        row = row + jnp.where(lane == t, jnp.sum(msk_ref[t:t + 1, :].astype(F32), axis=1, keepdims=True), 0.0)
    cnts[me] = row

    pl.semaphore_wait(bar, N_DEV - 1)

    def piece(slot, h, r0=0, n=DIM):
        return gx.at[slot, h, pl.ds(r0, n)]
    cuts = ((0, 0, 192), (0, 192, 192), (1, 0, 192), (1, 192, 128), (1, 320, 64))
    z_x = [rcopy(piece(OWN, *k), piece(FROM_Z, *k), to_zh, 0) for k in cuts]
    x_x = [rcopy(piece(OWN, h), piece(FROM_X, h), to_x, 0) for h in range(2)]
    y_x = [rcopy(piece(OWN, h), piece(FROM_Y, h), to_y, 0) for h in range(2)]
    xz_x = [rcopy(piece(FROM_Z, *k), piece(FROM_XZ, *k), to_x, 0) for k in cuts]
    yz_x = [rcopy(piece(FROM_Z, *k), piece(FROM_YZ, *k), to_y, 0) for k in cuts]
    z_e = rcopy(ge.at[OWN], ge.at[FROM_Z], to_zh, 1)
    x_e = rcopy(ge.at[OWN], ge.at[FROM_X], to_x, 1)
    y_e = rcopy(ge.at[OWN], ge.at[FROM_Y], to_y, 1)
    xz_e = rcopy(ge.at[FROM_Z], ge.at[FROM_XZ], to_x, 1)
    yz_e = rcopy(ge.at[FROM_Z], ge.at[FROM_YZ], to_y, 1)

    outer, inner = e == 0, e == 1

    def start_if(cond, cp):
        @pl.when(cond)
        def _():
            cp.start()

    def forward(got, a, b):
        got.wait_recv()
        start(a)
        start(b)

    exchange_start(cnts, ls.at[6], ls.at[7])
    start(z_x[0])
    start(x_x[0])
    start(y_x[0])

    for cp in loads[2:]:
        cp.wait()
    hp_ref[...] = jnp.zeros_like(hp_ref)
    for t in range(TASKS):
        hp_ref[PAD * t:PAD * t + CLS, :] = h_ref[t]

    def fwd(i, _):
        cols = pl.ds(pl.multiple_of(i * 256, 256), 256)
        p = dot(x_ref[...], w1_ref[:, cols])
        a_own[:, cols] = (p * gelu_cdf(p)[2]).astype(BF16)
        return 0
    lax.fori_loop(0, HID // 256, fwd, 0)
    start_if(inner, z_x[1])
    z = (x_ref[...].astype(F32) + dot(a_own[...], w2_ref[...])).astype(BF16)
    logits = dot_nt(hp_ref[...], z)
    cls = lax.broadcasted_iota(jnp.int32, (PAD, TOK), 0)
    valid = cls < CLS
    for t in range(TASKS):
        lg = jnp.where(valid, logits[PAD * t:PAD * (t + 1)], -jnp.inf)
        ex = jnp.exp(lg - jnp.max(lg, axis=0, keepdims=True))
        sm = ex / jnp.sum(ex, axis=0, keepdims=True)
        hot = (lab_ref[t:t + 1, :] == cls).astype(F32)
        ge[OWN, t] = jnp.where(valid, msk_ref[t:t + 1, :].astype(F32) * (sm - hot), 0.0).astype(BF16)
    start_if(inner, z_e)
    start_if(outer, z_x[1])
    start(x_e)
    start(y_e)
    start(x_x[1])
    start(y_x[1])

    hid_iota = lax.broadcasted_iota(jnp.int32, (DIM, HID), 1)
    seg = (col * 43691) >> 21
    src_a = 48 * ((seg >> 2) + 8 * (((seg >> 1) & 1) ^ zh) + 4 * (seg & 1) + 16 * zh + 2 * x) + (col - 48 * seg)
    seg = (col * 43691) >> 20
    src_b = (48 * (((seg >> 2) & 1) + 2 * ((seg >> 1) & 1) + 8 * ((seg & 1) ^ zh) + 16 * zh + 4 * y)
             + 24 * (seg >> 3) + (col - 24 * seg))
    for src, dst in ((src_a, w1a), (src_b, w1b)):
        sel = (hid_iota == src).astype(BF16)
        dst[...] = dot_nt(dot_nt(sel, w1_ref[...]).astype(BF16), perm).astype(BF16)
    for k in range(8):
        eb = (k >> 1) & 1
        dv = (k >> 2) + 8 * (eb + zh - 2 * eb * zh) + 4 * (k & 1) + 16 * zh + 2 * x
        w2a[48 * k:48 * (k + 1), :] = w2_ref[pl.ds(pl.multiple_of(48 * dv, 16), 48), :]
    for t in range(TASKS):
        ht[t] = jnp.transpose(hp_ref[PAD * t:PAD * (t + 1), :].astype(F32)).astype(BF16)

    strips = [slice(128 * r, 128 * (r + 1)) for r in range(3)]

    def slope(s, h):
        for rows in strips:
            p = dot(w1a[rows, :], gx[s, h])
            sq, t, cdf = gelu_cdf(p)
            gp[rows, :] = cdf + (0.5 * GELU_C) * p * (1.0 - t * t) * (1.0 + (3.0 * GELU_A) * sq)

    def act(s, h, k):
        for rows in strips:
            p = dot(w1b[rows, :], gx[s, h])
            at[k, h, rows, :] = (p * gelu_cdf(p)[2]).astype(BF16)

    def dz_of(s, h, t, ref):
        ref[...] = dot(ht[t], ge[s, t, :, HALF * h:HALF * (h + 1)]).astype(BF16)

    def q_of(h, t, k, ref):
        for rows in strips:
            qt[k, t, h, rows, :] = (dot(w2a[rows, :], ref[...]) * gp[rows, :]).astype(BF16)

    def prep_a(s, h, k):
        slope(s, h)
        for t in range(TASKS):
            dz_of(s, h, t, dzx)
            q_of(h, t, k, dzx)

    def prep_b(s, h, k):
        act(s, h, k)
        for t in range(TASKS):
            dz_of(s, h, t, dz.at[k, t, h])

    def prep(s, h):
        slope(s, h)
        act(s, h, 0)
        for t in range(TASKS):
            dz_of(s, h, t, dz.at[0, t, h])
            q_of(h, t, 0, dz.at[0, t, h])

    def add_a(s, t, k, first=False):
        d = dot_nt(gx[s, 0], qt[k, t, 0]) + dot_nt(gx[s, 1], qt[k, t, 1])
        d = (d * inv[t]).astype(BF16).astype(F32)
        acc1[t] = d if first else acc1[t] + d

    def add_b(t, k, first=False):
        d = dot_nt(at[k, 0], dz[k, t, 0]) + dot_nt(at[k, 1], dz[k, t, 1])
        d = (d * inv[t]).astype(BF16).astype(F32)
        acc2[t] = d if first else acc2[t] + d

    start_if(outer, z_e)
    start_if(inner, z_x[2])
    prep(OWN, 0)
    prep(OWN, 1)
    start_if(inner, z_x[3])
    exchange_wait(cnts, ls.at[7])
    total = jnp.sum(cnts[...], axis=0)
    recip = 1.0 / jnp.maximum(total, 1.0)
    for t in range(TASKS):
        inv[t] = jnp.broadcast_to(recip[:, t:t + 1], (1, DIM))
    for t in range(TASKS):
        add_a(OWN, t, 0, True)
        add_b(t, 0, True)
    start_if(inner, z_x[4])
    start_if(outer, z_x[2])
    for cp in (x_e, x_x[0], x_x[1]):
        cp.wait_recv()
    forward(z_x[0], xz_x[0], yz_x[0])
    prep_a(FROM_X, 0, 0)
    start_if(outer, z_x[3])
    forward(z_e, xz_e, yz_e)
    forward(z_x[1], xz_x[1], yz_x[1])
    prep_a(FROM_X, 1, 0)
    for t in range(TASKS):
        add_a(FROM_X, t, 0)
    start_if(outer, z_x[4])
    for cp in (y_e, y_x[0], y_x[1]):
        cp.wait_recv()
    prep_b(FROM_Y, 0, 0)
    prep_b(FROM_Y, 1, 0)
    for t in range(TASKS):
        add_b(t, 0)
    forward(z_x[2], xz_x[2], yz_x[2])
    prep(FROM_Z, 0)
    forward(z_x[3], xz_x[3], yz_x[3])
    forward(z_x[4], xz_x[4], yz_x[4])
    prep(FROM_Z, 1)
    for cp in (xz_e, xz_x[0], xz_x[1]):
        cp.wait_recv()
    prep_a(FROM_XZ, 0, 1)
    for cp in (yz_e, yz_x[0], yz_x[1]):
        cp.wait_recv()
    prep_b(FROM_YZ, 0, 1)
    add_a(FROM_Z, 0, 0)
    for cp in xz_x[2:]:
        cp.wait_recv()

    def rows(base, n):
        return pl.ds(pl.multiple_of(base, 8), n)
    bits1, bits2 = (c, y, e), (c, x, e)
    dest1, dest2 = (to_c, to_y, to_zl), (to_c, to_x, to_zl)
    z_first = ((0, 0),)

    def moves(bits, t, u, stage):
        at0 = 192 * u
        if stage == 0:
            return [(at0 + 96 * (1 - bits[0]), at0 + 96 * bits[0], 0, 96, 0)]
        at0 = at0 + 96 * bits[0]
        if (t, u) in z_first:
            if stage == 1:
                return [(at0 + 48 * b + 24 * (1 - bits[2]), at0 + 48 * b + 24 * bits[2], 24 * b, 24, 2) for b in range(2)]
            return [(at0 + 48 * (1 - bits[1]) + 24 * bits[2], at0 + 48 * bits[1] + 24 * bits[2], 0, 24, 1)]
        if stage == 1:
            return [(at0 + 48 * (1 - bits[1]), at0 + 48 * bits[1], 0, 48, 1)]
        at0 = at0 + 48 * bits[1]
        return [(at0 + 24 * (1 - bits[2]), at0 + 24 * bits[2], 0, 24, 2)]

    part1 = (acc1, (rc1, ra1, rb1), bits1, dest1)
    part2 = (acc2, (rc2, ra2, rb2), bits2, dest2)
    order = [(t, u) for t in range(TASKS) for u in range(2)]
    cps = {}

    def go(part, i, t, u, stage):
        acc, recv, bits, dest = part
        cps[i, t, u, stage] = [
            start(rcopy(acc.at[t, rows(out, n)], recv[stage].at[t, u, pl.ds(at0, n)], dest[link], 2 * stage + i + 1))
            for out, _, at0, n, link in moves(bits, t, u, stage)]

    def merge(part, t, u, stage):
        acc, recv, bits, _ = part
        for _, kept, at0, n, _ in moves(bits, t, u, stage):
            mine = rows(kept, n)
            v = acc[t, mine] + recv[stage][t, u, at0:at0 + n]
            acc[t, mine] = v
        return v

    def arrived(i, t, u, stage):
        for cp in cps[i, t, u, stage]:
            cp.wait_recv()

    def add(part, i, t, u, stage):
        arrived(i, t, u, stage)
        return merge(part, t, u, stage)

    own = 2 * zh + x
    fx, fz = 1 - 2 * x, 2 * (1 - 2 * zh)
    back = []

    for part in (pl.ds(0, 24), pl.ds(24, 16)):
        for dk, to in ((fz, to_zh), (fx + fz, to_x + to_zh - me), (fx, to_x)):
            back.append(rcopy(sb.at[own + dk, part], rb.at[own, part], to, 8))

    def send_back(which, cond):
        @pl.when(cond)
        def _():
            for cp in back[3 * which:3 * which + 3]:
                cp.start()

    def finish(t, u):
        g = add(part1, 1, t, u, 2)
        g1s[t, 24 * u:24 * (u + 1)] = g
        for k in range(2):
            sb[2 * u + k, 12 * t:12 * (t + 1)] = g[12 * k:12 * (k + 1)]
        g2s[t, 24 * u:24 * (u + 1)] = add(part2, 2, t, u, 2)

    both = ((1, part1), (2, part2))

    def first_hop(n):
        for i, part in both:
            add(part, i, *order[n], 0)
            go(part, i, *order[n], 1)

    slope(FROM_XZ, 1)
    for t in range(TASKS):
        dz_of(FROM_XZ, 1, t, dzx)
        q_of(1, t, 1, dzx)
        if t:
            add_a(FROM_Z, t, 0)
        add_a(FROM_XZ, t, 1)
        for u in range(2):
            go(part1, 1, t, u, 0)
        if t:
            first_hop(2 * t - 2)
        if t == 0:
            for cp in yz_x[2:]:
                cp.wait_recv()
            act(FROM_YZ, 1, 1)
        dz_of(FROM_YZ, 1, t, dz.at[1, t, 1])
        add_b(t, 0)
        add_b(t, 1)
        for u in range(2):
            go(part2, 2, t, u, 0)
        if t == 1:
            first_hop(1)
    sb[:, 36:40, :] = jnp.zeros((4, 4, DIM), F32)
    for n in range(6):
        if n + 3 < 6:
            for i, part in both:
                add(part, i, *order[n + 3], 0)
        for i, part in both:
            arrived(i, *order[n], 1)
            if n + 3 < 6:
                go(part, i, *order[n + 3], 1)
            merge(part, *order[n], 1)
            go(part, i, *order[n], 2)
        if n >= 3:
            finish(*order[n - 2])
    finish(*order[0])
    send_back(0, inner)
    finish(*order[4])
    send_back(0, outer)
    finish(*order[5])

    row = jnp.zeros((1, 128), F32)
    pairs = [(0, 0), (0, 1), (0, 2), (1, 1), (1, 2), (2, 2)]
    for i, (t, s) in enumerate(pairs):
        part = jnp.sum(g1s[t] * g1s[s] + g2s[t] * g2s[s], axis=0, keepdims=True)
        row = row + jnp.where(lane == i, jnp.sum(part, axis=1, keepdims=True), 0.0)
    grams[me] = row
    exchange_start(grams, ls.at[8], ls.at[9])
    for cp in back[3:]:
        cp.start()
    rb[own] = sb[own]
    for t in range(TASKS):
        for k in range(3):
            o2_ref[t, pl.ds(k, 48, stride=3), :] = g2s[t, :, 128 * k:128 * (k + 1)]
    for cp in back:
        cp.wait_recv()
    for t in range(TASKS):
        parts = []
        for b in range(32):
            bzh, bzl, by, bx, bc = b >> 4, (b >> 3) & 1, (b >> 2) & 1, (b >> 1) & 1, b & 1
            at0 = 192 * bc + 96 * (bzl ^ bzh) + 48 * by
            parts.append(rb[2 * bzh + bx, 12 * t:12 * (t + 1), at0:at0 + 48])
        full = jnp.concatenate(parts, axis=1)
        for k in range(12):
            o1_ref[t, pl.ds(k, 12, stride=12), :] = full[:, 128 * k:128 * (k + 1)]
    exchange_wait(grams, ls.at[9])
    m = jnp.sum(grams[...], axis=0)
    ent = [jnp.broadcast_to(m[:, i:i + 1], (8, 128)) for i in range(6)]
    neg = -TASKS / (ent[0] + ent[3] + ent[5])
    gram = {}
    for i, (t, s) in enumerate(pairs):
        gram[t, s] = gram[s, t] = ent[i] * neg
    w = [jnp.full((8, 128), 1.0 / TASKS, F32)] * TASKS
    for _ in range(SOLVER_STEPS):
        up = [w[t] * jnp.exp(gram[t, 0] * w[0] + gram[t, 1] * w[1] + gram[t, 2] * w[2]) for t in range(TASKS)]
        norm = 1.0 / (up[0] + up[1] + up[2])
        w = [v * norm for v in up]
    al_ref[...] = jnp.where(lane == 0, w[0][:1], jnp.where(lane == 1, w[1][:1], w[2][:1]))[:, :TASKS]
    exchange_wait(cnts, ls.at[6])
    exchange_wait(grams, ls.at[8])
    for i, ref in enumerate((gx.at[pl.ds(0, 5)], ge.at[pl.ds(0, 5)], rc1, rc2, ra1, ra2, rb1, rb2, rb.at[pl.ds(0, 3)])):
        wait_bytes(ref, ss.at[i])


def solution(mesh):
    def step(tokens, w_in, w_out, heads, lab, msk):
        vm = pl.BlockSpec(memory_space=pltpu.VMEM)
        dma = pltpu.SemaphoreType.DMA
        v = pltpu.VMEM
        alpha, g1, g2 = pl.pallas_call(
            kernel,
            name="step",
            out_shape=(jax.ShapeDtypeStruct((1, TASKS), F32), jax.ShapeDtypeStruct((TASKS, 144, 128), F32),
                       jax.ShapeDtypeStruct((TASKS, 144, 128), F32)),
            in_specs=[pl.BlockSpec(memory_space=pltpu.HBM)] * 6,
            out_specs=(vm, vm, vm),
            scratch_shapes=[
                v((TOK, DIM), BF16), v((DIM, HID), BF16), v((HID, DIM), BF16),
                v((TASKS, CLS, DIM), BF16), v((TASKS, TOK), jnp.int32),
                v((TASKS, TOK), jnp.int32), v((TASKS * PAD, DIM), BF16),
                v((N_DEV, 1, 128), F32), v((N_DEV, 1, 128), F32),
                v((6, 2, DIM, HALF), BF16), v((6, TASKS, PAD, TOK), BF16),
                v((TASKS, DIM, PAD), BF16), v((DIM, DIM), BF16), v((DIM, DIM), BF16), v((DIM, DIM), BF16),
                v((TOK, HID), BF16), v((2, 2, DIM, HALF), BF16), v((DIM, HALF), F32),
                v((2, TASKS, 2, DIM, HALF), BF16), v((DIM, HALF), BF16), v((2, TASKS, 2, DIM, HALF), BF16),
                v((TASKS, 1, DIM), F32),
                v((TASKS, DIM, DIM), F32), v((TASKS, DIM, DIM), F32),
                v((TASKS, 2, 96, DIM), F32), v((TASKS, 2, 96, DIM), F32),
                v((TASKS, 2, 48, DIM), F32), v((TASKS, 2, 48, DIM), F32),
                v((TASKS, 2, 24, DIM), F32), v((TASKS, 2, 24, DIM), F32),
                v((TASKS, 48, DIM), F32), v((TASKS, 48, DIM), F32),
                v((4, 40, DIM), F32), v((4, 40, DIM), F32),
                dma((9,)), dma((N_SEM,)), dma((10,)),
            ],
            compiler_params=pltpu.CompilerParams(collective_id=0, has_side_effects=True, vmem_limit_bytes=28 * 2**20),
        )(*[pltpu.with_memory_space_constraint(a, pltpu.HBM)
            for a in (tokens, w_in, w_out, heads.transpose(0, 2, 1), lab, msk)])
        alpha = alpha.reshape(TASKS)
        w = alpha[:, None, None]
        return alpha, (w * g1).sum(axis=0).reshape(-1), (w * g2).sum(axis=0).reshape(-1)

    return jax.shard_map(step, mesh=mesh, in_specs=(P("data", None), P(), P(), P(), P(None, "data"), P(None, "data")),
                         out_specs=(P(), P("data"), P("data")), check_vma=False)
```

```python
import jax
import jax.numpy as jnp
from jax import lax
from jax.experimental import pallas as pl
from jax.experimental.pallas import tpu as pltpu
from jax.sharding import PartitionSpec as P

MESH = pl.DeviceIdType.MESH
SOLVER_STEPS = 20
N_DEV = 32
TOK, DIM, HID, TASKS, CLS, PAD = 512, 384, 1536, 3, 13, 16
HALF = TOK // 2
GELU_C = 0.7978845608028654
GELU_A = 0.044715
N_SEM = 66
OWN, FROM_X, FROM_Z, FROM_XZ, FROM_Y, FROM_YZ = range(6)

F32, BF16 = jnp.float32, jnp.bfloat16


def dot(a, b):
    return jnp.dot(a, b, preferred_element_type=F32)


def dot_nt(a, b):
    return lax.dot_general(a, b, (((1,), (1,)), ((), ())), preferred_element_type=F32)


def bit(v, i):
    return (v >> i) & 1


def flip(b):
    return 1 - 2 * b


def index(c, x, y, zl, zh):
    return c + 2 * x + 4 * y + 8 * zl + 16 * zh


def tile(k, n=128):
    return slice(n * k, n * (k + 1))


def gelu_cdf(p):
    sq = p * p
    t = jnp.tanh(GELU_C * (p + GELU_A * (sq * p)))
    return sq, t, 0.5 * (1.0 + t)


def kernel(x_hbm, w1_hbm, w2_hbm, h_hbm, lab_hbm, msk_hbm, al_ref, o1_ref, o2_ref,
           x_ref, w1_ref, w2_ref, h_ref, lab_ref, msk_ref, hp_ref, cnts, grams,
           gx, ge, ht, w1a, w1b, w2a, a_own, at, gp, dz, dzx, qt, inv, acc1, acc2,
           rc1, rc2, ra1, ra2, rb1, rb2, g1s, g2s, sb, rb,
           ss, rs, ls):
    me = lax.axis_index("data")
    c, x, y, zl, zh = (lax.rem(me // n, 2) for n in (1, 2, 4, 8, 16))
    to_c, to_x, to_y = me + flip(c), me + 2 * flip(x), me + 4 * flip(y)
    to_zh = me + index(0, 0, 0, flip(zl), flip(zh))
    e = lax.rem(zh + zl, 2)
    to_zl = me + 8 * flip(zl)

    used = []

    def rcopy(src, dst, dev, group):
        i = len(used)
        used.append(i)
        return pltpu.make_async_remote_copy(src_ref=src, dst_ref=dst, send_sem=ss.at[group], recv_sem=rs.at[i],
                                            device_id=(dev,), device_id_type=MESH)

    def start(cp):
        cp.start()
        return cp

    def wait_bytes(ref, sem):
        pltpu.make_async_copy(ref, ref, sem).wait()

    def row_copy(buf, src_row, send_sem, recv_sem, dev):
        return pltpu.make_async_remote_copy(src_ref=buf.at[src_row], dst_ref=buf.at[src_row], send_sem=send_sem,
                                            recv_sem=recv_sem, device_id=(dev,), device_id_type=MESH)

    def exchange_start(buf, s_sem, r_sem):
        def go(i, _):
            row_copy(buf, me, s_sem, r_sem, lax.rem(me + i, N_DEV)).start()
            return 0
        lax.fori_loop(1, N_DEV, go, 0)

    def exchange_wait(buf, sem):
        wait_bytes(buf.at[pl.ds(0, N_DEV - 1)], sem)

    loads = [pltpu.make_async_copy(a, b, ls.at[i]) for i, (a, b) in enumerate((
        (x_hbm, x_ref), (msk_hbm, msk_ref), (w1_hbm, w1_ref), (w2_hbm, w2_ref), (h_hbm, h_ref), (lab_hbm, lab_ref)))]
    for cp in loads:
        cp.start()

    bar = pltpu.get_barrier_semaphore()

    def sig(i, _):
        pl.semaphore_signal(bar, inc=1, device_id=(lax.rem(me + i, N_DEV),), device_id_type=MESH)
        return 0
    lax.fori_loop(1, N_DEV, sig, 0)

    col = lax.broadcasted_iota(jnp.int32, (DIM, 1), 0)
    blk = (col * 43691) >> 19
    dev = index(bit(blk, 3), bit(blk, 0), bit(blk, 2), bit(blk, 1) ^ bit(blk, 4), bit(blk, 4))
    perm = (lax.broadcasted_iota(jnp.int32, (DIM, DIM), 1) == 12 * dev + (col - 12 * blk)).astype(BF16)
    loads[0].wait()
    for h in range(2):
        gx[OWN, h] = dot_nt(perm, x_ref[tile(h, HALF), :]).astype(BF16)
    lane = lax.broadcasted_iota(jnp.int32, (1, 128), 1)
    row = jnp.zeros((1, 128), F32)
    loads[1].wait()
    for t in range(TASKS):
        row = row + jnp.where(lane == t, jnp.sum(msk_ref[t:t + 1, :].astype(F32), axis=1, keepdims=True), 0.0)
    cnts[me] = row

    pl.semaphore_wait(bar, N_DEV - 1)

    def piece(slot, h, r0=0, n=DIM):
        return gx.at[slot, h, pl.ds(r0, n)]
    cuts = ((0, 0, 192), (0, 192, 192), (1, 0, 192), (1, 192, 128), (1, 320, 64))
    z_x = [rcopy(piece(OWN, *k), piece(FROM_Z, *k), to_zh, 0) for k in cuts]
    x_x = [rcopy(piece(OWN, h), piece(FROM_X, h), to_x, 0) for h in range(2)]
    y_x = [rcopy(piece(OWN, h), piece(FROM_Y, h), to_y, 0) for h in range(2)]
    xz_x = [rcopy(piece(FROM_Z, *k), piece(FROM_XZ, *k), to_x, 0) for k in cuts]
    yz_x = [rcopy(piece(FROM_Z, *k), piece(FROM_YZ, *k), to_y, 0) for k in cuts]
    z_e = rcopy(ge.at[OWN], ge.at[FROM_Z], to_zh, 1)
    x_e = rcopy(ge.at[OWN], ge.at[FROM_X], to_x, 1)
    y_e = rcopy(ge.at[OWN], ge.at[FROM_Y], to_y, 1)
    xz_e = rcopy(ge.at[FROM_Z], ge.at[FROM_XZ], to_x, 1)
    yz_e = rcopy(ge.at[FROM_Z], ge.at[FROM_YZ], to_y, 1)

    outer, inner = e == 0, e == 1

    def start_if(cond, cp):
        @pl.when(cond)
        def _():
            cp.start()

    def forward(got, a, b):
        got.wait_recv()
        start(a)
        start(b)

    exchange_start(cnts, ls.at[6], ls.at[7])
    start(z_x[0])
    start(x_x[0])
    start(y_x[0])

    for cp in loads[2:]:
        cp.wait()
    hp_ref[...] = jnp.zeros_like(hp_ref)
    for t in range(TASKS):
        hp_ref[PAD * t:PAD * t + CLS, :] = h_ref[t]

    def fwd(i, _):
        cols = pl.ds(pl.multiple_of(i * 256, 256), 256)
        p = dot(x_ref[...], w1_ref[:, cols])
        a_own[:, cols] = (p * gelu_cdf(p)[2]).astype(BF16)
        return 0
    lax.fori_loop(0, HID // 256, fwd, 0)
    start_if(inner, z_x[1])
    z = (x_ref[...].astype(F32) + dot(a_own[...], w2_ref[...])).astype(BF16)
    logits = dot_nt(hp_ref[...], z)
    cls = lax.broadcasted_iota(jnp.int32, (PAD, TOK), 0)
    valid = cls < CLS
    for t in range(TASKS):
        lg = jnp.where(valid, logits[tile(t, PAD)], -jnp.inf)
        ex = jnp.exp(lg - jnp.max(lg, axis=0, keepdims=True))
        sm = ex / jnp.sum(ex, axis=0, keepdims=True)
        hot = (lab_ref[t:t + 1, :] == cls).astype(F32)
        ge[OWN, t] = jnp.where(valid, msk_ref[t:t + 1, :].astype(F32) * (sm - hot), 0.0).astype(BF16)
    start_if(inner, z_e)
    start_if(outer, z_x[1])
    start(x_e)
    start(y_e)
    start(x_x[1])
    start(y_x[1])

    hid_iota = lax.broadcasted_iota(jnp.int32, (DIM, HID), 1)
    seg = (col * 43691) >> 21
    src_a = 48 * (index(bit(seg, 2), x, bit(seg, 0), bit(seg, 1) ^ zh, zh) - seg) + col
    seg = (col * 43691) >> 20
    src_b = 48 * index(bit(seg, 2), bit(seg, 1), y, bit(seg, 0) ^ zh, zh) + 24 * (bit(seg, 3) - seg) + col
    for src, dst in ((src_a, w1a), (src_b, w1b)):
        sel = (hid_iota == src).astype(BF16)
        dst[...] = dot_nt(dot_nt(sel, w1_ref[...]).astype(BF16), perm).astype(BF16)
    for k in range(8):
        dv = index(bit(k, 2), x, bit(k, 0), bit(k, 1) * flip(zh) + zh, zh)
        w2a[tile(k, 48), :] = w2_ref[pl.ds(pl.multiple_of(48 * dv, 16), 48), :]
    for t in range(TASKS):
        ht[t] = jnp.transpose(hp_ref[tile(t, PAD), :].astype(F32)).astype(BF16)

    strips = [tile(r) for r in range(TASKS)]

    def slope(s, h):
        for rows in strips:
            p = dot(w1a[rows, :], gx[s, h])
            sq, t, cdf = gelu_cdf(p)
            gp[rows, :] = cdf + (0.5 * GELU_C) * p * (1.0 - t * t) * (1.0 + (3.0 * GELU_A) * sq)

    def act(s, h, k):
        for rows in strips:
            p = dot(w1b[rows, :], gx[s, h])
            at[k, h, rows, :] = (p * gelu_cdf(p)[2]).astype(BF16)

    def dz_of(s, h, t, ref):
        ref[...] = dot(ht[t], ge[s, t, :, tile(h, HALF)]).astype(BF16)

    def q_of(h, t, k, ref):
        for rows in strips:
            qt[k, t, h, rows, :] = (dot(w2a[rows, :], ref[...]) * gp[rows, :]).astype(BF16)

    def prep_a(s, h, k):
        slope(s, h)
        for t in range(TASKS):
            dz_of(s, h, t, dzx)
            q_of(h, t, k, dzx)

    def prep_b(s, h, k):
        act(s, h, k)
        for t in range(TASKS):
            dz_of(s, h, t, dz.at[k, t, h])

    def prep(s, h):
        slope(s, h)
        act(s, h, 0)
        for t in range(TASKS):
            dz_of(s, h, t, dz.at[0, t, h])
            q_of(h, t, 0, dz.at[0, t, h])

    def add_a(s, t, k, first=False):
        d = dot_nt(gx[s, 0], qt[k, t, 0]) + dot_nt(gx[s, 1], qt[k, t, 1])
        d = (d * inv[t]).astype(BF16).astype(F32)
        acc1[t] = d if first else acc1[t] + d

    def add_b(t, k, first=False):
        d = dot_nt(at[k, 0], dz[k, t, 0]) + dot_nt(at[k, 1], dz[k, t, 1])
        d = (d * inv[t]).astype(BF16).astype(F32)
        acc2[t] = d if first else acc2[t] + d

    start_if(outer, z_e)
    start_if(inner, z_x[2])
    prep(OWN, 0)
    prep(OWN, 1)
    start_if(inner, z_x[3])
    exchange_wait(cnts, ls.at[7])
    total = jnp.sum(cnts[...], axis=0)
    recip = 1.0 / jnp.maximum(total, 1.0)
    for t in range(TASKS):
        inv[t] = jnp.broadcast_to(recip[:, t:t + 1], (1, DIM))
    for t in range(TASKS):
        add_a(OWN, t, 0, True)
        add_b(t, 0, True)
    start_if(inner, z_x[4])
    start_if(outer, z_x[2])
    start_if(outer, z_x[3])
    for cp in (x_e, x_x[0], x_x[1]):
        cp.wait_recv()
    forward(z_x[0], xz_x[0], yz_x[0])
    prep_a(FROM_X, 0, 0)
    start_if(outer, z_x[4])
    forward(z_e, xz_e, yz_e)
    forward(z_x[1], xz_x[1], yz_x[1])
    prep_a(FROM_X, 1, 0)
    for t in range(TASKS):
        add_a(FROM_X, t, 0)
    for cp in (y_e, y_x[0], y_x[1]):
        cp.wait_recv()
    prep_b(FROM_Y, 0, 0)
    prep_b(FROM_Y, 1, 0)
    for t in range(TASKS):
        add_b(t, 0)
    forward(z_x[2], xz_x[2], yz_x[2])
    prep(FROM_Z, 0)
    forward(z_x[3], xz_x[3], yz_x[3])
    forward(z_x[4], xz_x[4], yz_x[4])
    prep(FROM_Z, 1)
    for cp in (xz_e, xz_x[0], xz_x[1]):
        cp.wait_recv()
    prep_a(FROM_XZ, 0, 1)
    for cp in (yz_e, yz_x[0], yz_x[1]):
        cp.wait_recv()
    prep_b(FROM_YZ, 0, 1)
    add_a(FROM_Z, 0, 0)
    for cp in xz_x[2:]:
        cp.wait_recv()

    def rows(base, n):
        return pl.ds(pl.multiple_of(base, 8), n)
    bits1, bits2 = (c, y, e), (c, x, e)
    dest1, dest2 = (to_c, to_y, to_zl), (to_c, to_x, to_zl)

    def moves(bits, u, stage):
        bc, bm, be = bits

        def pick(at0, b, n):
            return at0 + n * (1 - b), at0 + n * b, n
        at0 = 192 * u
        if stage == 0:
            return pick(at0, bc, 96)
        at0 = at0 + 96 * bc
        if stage == 1:
            return pick(at0, bm, 48)
        return pick(at0 + 48 * bm, be, 24)

    part1 = (acc1, (rc1, ra1, rb1), bits1, dest1)
    part2 = (acc2, (rc2, ra2, rb2), bits2, dest2)
    order = [(t, u) for t in range(TASKS) for u in range(2)]
    cps = {}

    def go(part, i, t, u, stage):
        acc, recv, bits, dest = part
        out, _, n = moves(bits, u, stage)
        cps[i, t, u, stage] = start(
            rcopy(acc.at[t, rows(out, n)], recv[stage].at[t, u], dest[stage], 2 * stage + i + 1))

    def merge(part, t, u, stage):
        acc, recv, bits, _ = part
        _, kept, n = moves(bits, u, stage)
        v = acc[t, rows(kept, n)] + recv[stage][t, u]
        acc[t, rows(kept, n)] = v
        return v

    def add(part, i, t, u, stage):
        cps[i, t, u, stage].wait_recv()
        return merge(part, t, u, stage)

    own = 2 * zh + x
    fx, fz = flip(x), 2 * flip(zh)
    back = []

    for part in (pl.ds(0, 24), pl.ds(24, 16)):
        for dk, to in ((fz, to_zh), (fx + fz, to_x + to_zh - me), (fx, to_x)):
            back.append(rcopy(sb.at[own + dk, part], rb.at[own, part], to, 8))

    def send_back(which, cond):
        @pl.when(cond)
        def _():
            for cp in back[3 * which:3 * which + 3]:
                cp.start()

    def finish(t, u):
        g = add(part1, 1, t, u, 2)
        g1s[t, tile(u, 24)] = g
        for k in range(2):
            sb[2 * u + k, tile(t, 12)] = g[tile(k, 12)]
        g2s[t, tile(u, 24)] = add(part2, 2, t, u, 2)

    both = ((1, part1), (2, part2))

    def first_hop(n):
        for i, part in both:
            add(part, i, *order[n], 0)
            go(part, i, *order[n], 1)

    slope(FROM_XZ, 1)
    for t in range(TASKS):
        dz_of(FROM_XZ, 1, t, dzx)
        q_of(1, t, 1, dzx)
        if t:
            add_a(FROM_Z, t, 0)
        add_a(FROM_XZ, t, 1)
        for u in range(2):
            go(part1, 1, t, u, 0)
        if t:
            first_hop(2 * t - 2)
        if t == 0:
            for cp in yz_x[2:]:
                cp.wait_recv()
            act(FROM_YZ, 1, 1)
        dz_of(FROM_YZ, 1, t, dz.at[1, t, 1])
        add_b(t, 0)
        add_b(t, 1)
        for u in range(2):
            go(part2, 2, t, u, 0)
        if t == 1:
            first_hop(1)
    sb[:, 36:40, :] = jnp.zeros((4, 4, DIM), F32)
    for n in range(6):
        if n + 3 < 6:
            for i, part in both:
                add(part, i, *order[n + 3], 0)
        for i, part in both:
            cps[i, *order[n], 1].wait_recv()
            if n + 3 < 6:
                go(part, i, *order[n + 3], 1)
            merge(part, *order[n], 1)
            go(part, i, *order[n], 2)
        if n >= 2:
            finish(*order[n - 2])
    send_back(0, inner)
    finish(*order[4])
    send_back(0, outer)
    finish(*order[5])

    row = jnp.zeros((1, 128), F32)
    pairs = [(t, s) for t in range(TASKS) for s in range(t, TASKS)]
    for i, (t, s) in enumerate(pairs):
        part = jnp.sum(g1s[t] * g1s[s] + g2s[t] * g2s[s], axis=0, keepdims=True)
        row = row + jnp.where(lane == i, jnp.sum(part, axis=1, keepdims=True), 0.0)
    grams[me] = row
    exchange_start(grams, ls.at[8], ls.at[9])
    for cp in back[3:]:
        cp.start()
    rb[own] = sb[own]
    for t in range(TASKS):
        for k in range(3):
            o2_ref[t, pl.ds(k, 48, stride=3), :] = g2s[t, :, tile(k)]
    for cp in back:
        cp.wait_recv()
    for t in range(TASKS):
        parts = []
        for b in range(32):
            bc, bx, by, bzl, bzh = (bit(b, i) for i in range(5))
            at0 = 192 * bc + 96 * (bzl ^ bzh) + 48 * by
            parts.append(rb[2 * bzh + bx, tile(t, 12), at0:at0 + 48])
        full = jnp.concatenate(parts, axis=1)
        for k in range(12):
            o1_ref[t, pl.ds(k, 12, stride=12), :] = full[:, tile(k)]
    exchange_wait(grams, ls.at[9])
    m = jnp.sum(grams[...], axis=0)
    ent = [jnp.broadcast_to(m[:, i:i + 1], (8, 128)) for i in range(6)]
    neg = -TASKS / sum(ent[i] for i, (t, s) in enumerate(pairs) if t == s)
    gram = {}
    for i, (t, s) in enumerate(pairs):
        gram[t, s] = gram[s, t] = ent[i] * neg
    w = [jnp.full((8, 128), 1.0 / TASKS, F32)] * TASKS
    for _ in range(SOLVER_STEPS):
        up = [w[t] * jnp.exp(sum(gram[t, s] * w[s] for s in range(TASKS))) for t in range(TASKS)]
        norm = 1.0 / sum(up)
        w = [v * norm for v in up]
    al_ref[...] = sum(jnp.where(lane == t, w[t][:1], 0.0) for t in range(TASKS))[:, :TASKS]
    exchange_wait(cnts, ls.at[6])
    exchange_wait(grams, ls.at[8])
    for i, ref in enumerate((gx.at[pl.ds(0, 5)], ge.at[pl.ds(0, 5)], rc1, rc2, ra1, ra2, rb1, rb2, rb.at[pl.ds(0, 3)])):
        wait_bytes(ref, ss.at[i])


def solution(mesh):
    def step(tokens, w_in, w_out, heads, lab, msk):
        vm = pl.BlockSpec(memory_space=pltpu.VMEM)
        dma = pltpu.SemaphoreType.DMA
        v = pltpu.VMEM
        alpha, g1, g2 = pl.pallas_call(
            kernel,
            name="step",
            out_shape=(jax.ShapeDtypeStruct((1, TASKS), F32), jax.ShapeDtypeStruct((TASKS, 144, 128), F32),
                       jax.ShapeDtypeStruct((TASKS, 144, 128), F32)),
            in_specs=[pl.BlockSpec(memory_space=pltpu.HBM)] * 6,
            out_specs=(vm, vm, vm),
            scratch_shapes=[
                v((TOK, DIM), BF16), v((DIM, HID), BF16), v((HID, DIM), BF16),
                v((TASKS, CLS, DIM), BF16), v((TASKS, TOK), jnp.int32),
                v((TASKS, TOK), jnp.int32), v((TASKS * PAD, DIM), BF16),
                v((N_DEV, 1, 128), F32), v((N_DEV, 1, 128), F32),
                v((6, 2, DIM, HALF), BF16), v((6, TASKS, PAD, TOK), BF16),
                v((TASKS, DIM, PAD), BF16), v((DIM, DIM), BF16), v((DIM, DIM), BF16), v((DIM, DIM), BF16),
                v((TOK, HID), BF16), v((2, 2, DIM, HALF), BF16), v((DIM, HALF), F32),
                v((2, TASKS, 2, DIM, HALF), BF16), v((DIM, HALF), BF16), v((2, TASKS, 2, DIM, HALF), BF16),
                v((TASKS, 1, DIM), F32),
                v((TASKS, DIM, DIM), F32), v((TASKS, DIM, DIM), F32),
                v((TASKS, 2, 96, DIM), F32), v((TASKS, 2, 96, DIM), F32),
                v((TASKS, 2, 48, DIM), F32), v((TASKS, 2, 48, DIM), F32),
                v((TASKS, 2, 24, DIM), F32), v((TASKS, 2, 24, DIM), F32),
                v((TASKS, 48, DIM), F32), v((TASKS, 48, DIM), F32),
                v((4, 40, DIM), F32), v((4, 40, DIM), F32),
                dma((9,)), dma((N_SEM,)), dma((10,)),
            ],
            compiler_params=pltpu.CompilerParams(collective_id=0, has_side_effects=True, vmem_limit_bytes=28 * 2**20),
        )(*[pltpu.with_memory_space_constraint(a, pltpu.HBM)
            for a in (tokens, w_in, w_out, heads.transpose(0, 2, 1), lab, msk)])
        alpha = alpha.reshape(TASKS)
        w = alpha[:, None, None]
        return alpha, (w * g1).sum(axis=0).reshape(-1), (w * g2).sum(axis=0).reshape(-1)

    return jax.shard_map(step, mesh=mesh, in_specs=(P("data", None), P(), P(), P(), P(None, "data"), P(None, "data")),
                         out_specs=(P(), P("data"), P("data")), check_vma=False)
```

```python
import jax
import jax.numpy as jnp
from jax import lax
from jax.experimental import pallas as pl
from jax.experimental.pallas import tpu as pltpu
from jax.sharding import PartitionSpec as P

MESH = pl.DeviceIdType.MESH
SOLVER_STEPS = 20
N_DEV = 32
TOK, DIM, HID, TASKS, CLS, PAD = 512, 384, 1536, 3, 13, 16
HALF = TOK // 2
GELU_C = 0.7978845608028654
GELU_A = 0.044715
N_SEM = 66
OWN, FROM_X, FROM_Z, FROM_XZ, FROM_Y, FROM_YZ = range(6)

F32, BF16 = jnp.float32, jnp.bfloat16


def dot(a, b):
    return jnp.dot(a, b, preferred_element_type=F32)


def dot_nt(a, b):
    return lax.dot_general(a, b, (((1,), (1,)), ((), ())), preferred_element_type=F32)


def bit(v, i):
    return (v >> i) & 1


def flip(b):
    return 1 - 2 * b


def index(c, x, y, zl, zh):
    return c + 2 * x + 4 * y + 8 * zl + 16 * zh


def tile(k, n=128):
    return slice(n * k, n * (k + 1))


def gelu_cdf(p):
    sq = p * p
    t = jnp.tanh(GELU_C * (p + GELU_A * (sq * p)))
    return sq, t, 0.5 * (1.0 + t)


def kernel(x_hbm, w1_hbm, w2_hbm, h_hbm, lab_hbm, msk_hbm, al_ref, o1_ref, o2_ref,
           x_ref, w1_ref, w2_ref, h_ref, lab_ref, msk_ref, hp_ref, cnts, grams,
           gx, ge, ht, w1a, w1b, w2a, a_own, at, gp, dz, dzx, qt, inv, acc1, acc2,
           rc1, rc2, ra1, ra2, rb1, rb2, g1s, g2s, sb, rb,
           ss, rs, ls):
    me = lax.axis_index("data")
    c, x, y, zl, zh = (lax.rem(me // n, 2) for n in (1, 2, 4, 8, 16))
    to_c, to_x, to_y = me + flip(c), me + 2 * flip(x), me + 4 * flip(y)
    to_zh = me + index(0, 0, 0, flip(zl), flip(zh))
    e = lax.rem(zh + zl, 2)
    to_zl = me + 8 * flip(zl)

    used = []

    def rcopy(src, dst, dev, group):
        i = len(used)
        used.append(i)
        return pltpu.make_async_remote_copy(src_ref=src, dst_ref=dst, send_sem=ss.at[group], recv_sem=rs.at[i],
                                            device_id=(dev,), device_id_type=MESH)

    def start(cp):
        cp.start()
        return cp

    def wait_bytes(ref, sem):
        pltpu.make_async_copy(ref, ref, sem).wait()

    def row_copy(buf, src_row, send_sem, recv_sem, dev):
        return pltpu.make_async_remote_copy(src_ref=buf.at[src_row], dst_ref=buf.at[src_row], send_sem=send_sem,
                                            recv_sem=recv_sem, device_id=(dev,), device_id_type=MESH)

    def exchange_start(buf, s_sem, r_sem):
        def go(i, _):
            row_copy(buf, me, s_sem, r_sem, lax.rem(me + i, N_DEV)).start()
            return 0
        lax.fori_loop(1, N_DEV, go, 0)

    def exchange_wait(buf, sem):
        wait_bytes(buf.at[pl.ds(0, N_DEV - 1)], sem)

    loads = [pltpu.make_async_copy(a, b, ls.at[i]) for i, (a, b) in enumerate((
        (x_hbm, x_ref), (msk_hbm, msk_ref), (w1_hbm, w1_ref), (w2_hbm, w2_ref), (h_hbm, h_ref), (lab_hbm, lab_ref)))]
    for cp in loads:
        cp.start()

    bar = pltpu.get_barrier_semaphore()

    def sig(i, _):
        pl.semaphore_signal(bar, inc=1, device_id=(lax.rem(me + i, N_DEV),), device_id_type=MESH)
        return 0
    lax.fori_loop(1, N_DEV, sig, 0)

    col = lax.broadcasted_iota(jnp.int32, (DIM, 1), 0)
    blk = (col * 43691) >> 19
    dev = index(bit(blk, 3), bit(blk, 0), bit(blk, 2), bit(blk, 1) ^ bit(blk, 4), bit(blk, 4))
    perm = (lax.broadcasted_iota(jnp.int32, (DIM, DIM), 1) == 12 * dev + (col - 12 * blk)).astype(BF16)
    loads[0].wait()
    for h in range(2):
        gx[OWN, h] = dot_nt(perm, x_ref[tile(h, HALF), :]).astype(BF16)
    lane = lax.broadcasted_iota(jnp.int32, (1, 128), 1)
    row = jnp.zeros((1, 128), F32)
    loads[1].wait()
    for t in range(TASKS):
        row = row + jnp.where(lane == t, jnp.sum(msk_ref[t:t + 1, :].astype(F32), axis=1, keepdims=True), 0.0)
    cnts[me] = row

    pl.semaphore_wait(bar, N_DEV - 1)

    def piece(slot, h, r0=0, n=DIM):
        return gx.at[slot, h, pl.ds(r0, n)]
    cuts = ((0, 0, 192), (0, 192, 192), (1, 0, 192), (1, 192, 96), (1, 288, 96))
    z_x = [rcopy(piece(OWN, *k), piece(FROM_Z, *k), to_zh, 0) for k in cuts]
    x_x = [rcopy(piece(OWN, h), piece(FROM_X, h), to_x, 0) for h in range(2)]
    y_x = [rcopy(piece(OWN, h), piece(FROM_Y, h), to_y, 0) for h in range(2)]
    xz_x = [rcopy(piece(FROM_Z, *k), piece(FROM_XZ, *k), to_x, 0) for k in cuts]
    yz_x = [rcopy(piece(FROM_Z, *k), piece(FROM_YZ, *k), to_y, 0) for k in cuts]
    z_e = rcopy(ge.at[OWN], ge.at[FROM_Z], to_zh, 1)
    x_e = rcopy(ge.at[OWN], ge.at[FROM_X], to_x, 1)
    y_e = rcopy(ge.at[OWN], ge.at[FROM_Y], to_y, 1)
    xz_e = rcopy(ge.at[FROM_Z], ge.at[FROM_XZ], to_x, 1)
    yz_e = rcopy(ge.at[FROM_Z], ge.at[FROM_YZ], to_y, 1)

    outer, inner = e == 0, e == 1

    def start_if(cond, cp):
        @pl.when(cond)
        def _():
            cp.start()

    def forward(got, a, b):
        got.wait_recv()
        start(a)
        start(b)

    exchange_start(cnts, ls.at[6], ls.at[7])
    start(z_x[0])
    start(x_x[0])
    start(y_x[0])

    for cp in loads[2:]:
        cp.wait()
    hp_ref[...] = jnp.zeros_like(hp_ref)
    for t in range(TASKS):
        hp_ref[PAD * t:PAD * t + CLS, :] = h_ref[t]

    def fwd(i, _):
        cols = pl.ds(pl.multiple_of(i * 256, 256), 256)
        p = dot(x_ref[...], w1_ref[:, cols])
        a_own[:, cols] = (p * gelu_cdf(p)[2]).astype(BF16)
        return 0
    lax.fori_loop(0, HID // 256, fwd, 0)
    start_if(inner, z_x[1])
    z = (x_ref[...].astype(F32) + dot(a_own[...], w2_ref[...])).astype(BF16)
    logits = dot_nt(hp_ref[...], z)
    cls = lax.broadcasted_iota(jnp.int32, (PAD, TOK), 0)
    valid = cls < CLS
    for t in range(TASKS):
        lg = jnp.where(valid, logits[tile(t, PAD)], -jnp.inf)
        ex = jnp.exp(lg - jnp.max(lg, axis=0, keepdims=True))
        sm = ex / jnp.sum(ex, axis=0, keepdims=True)
        hot = (lab_ref[t:t + 1, :] == cls).astype(F32)
        ge[OWN, t] = jnp.where(valid, msk_ref[t:t + 1, :].astype(F32) * (sm - hot), 0.0).astype(BF16)
    start_if(inner, z_e)
    start_if(outer, z_x[1])
    start(x_e)
    start(y_e)
    start(x_x[1])
    start(y_x[1])

    hid_iota = lax.broadcasted_iota(jnp.int32, (DIM, HID), 1)
    seg = (col * 43691) >> 21
    src_a = 48 * (index(bit(seg, 2), x, bit(seg, 0), bit(seg, 1) ^ zh, zh) - seg) + col
    seg = (col * 43691) >> 20
    src_b = 48 * index(bit(seg, 2), bit(seg, 1), y, bit(seg, 0) ^ zh, zh) + 24 * (bit(seg, 3) - seg) + col
    for src, dst in ((src_a, w1a), (src_b, w1b)):
        sel = (hid_iota == src).astype(BF16)
        dst[...] = dot_nt(dot_nt(sel, w1_ref[...]).astype(BF16), perm).astype(BF16)
    for k in range(8):
        dv = index(bit(k, 2), x, bit(k, 0), bit(k, 1) * flip(zh) + zh, zh)
        w2a[tile(k, 48), :] = w2_ref[pl.ds(pl.multiple_of(48 * dv, 16), 48), :]
    for t in range(TASKS):
        ht[t] = jnp.transpose(hp_ref[tile(t, PAD), :].astype(F32)).astype(BF16)

    strips = [tile(r) for r in range(TASKS)]

    def slope(s, h):
        for rows in strips:
            p = dot(w1a[rows, :], gx[s, h])
            sq, t, cdf = gelu_cdf(p)
            gp[rows, :] = cdf + (0.5 * GELU_C) * p * (1.0 - t * t) * (1.0 + (3.0 * GELU_A) * sq)

    def act(s, h, k):
        for rows in strips:
            p = dot(w1b[rows, :], gx[s, h])
            at[k, h, rows, :] = (p * gelu_cdf(p)[2]).astype(BF16)

    def dz_of(s, h, t, ref):
        ref[...] = dot(ht[t], ge[s, t, :, tile(h, HALF)]).astype(BF16)

    def q_of(h, t, k, ref):
        for rows in strips:
            qt[k, t, h, rows, :] = (dot(w2a[rows, :], ref[...]) * gp[rows, :]).astype(BF16)

    def prep_a(s, h, k):
        slope(s, h)
        for t in range(TASKS):
            dz_of(s, h, t, dzx)
            q_of(h, t, k, dzx)

    def prep_b(s, h, k):
        act(s, h, k)
        for t in range(TASKS):
            dz_of(s, h, t, dz.at[k, t, h])

    def prep(s, h):
        slope(s, h)
        act(s, h, 0)
        for t in range(TASKS):
            dz_of(s, h, t, dz.at[0, t, h])
            q_of(h, t, 0, dz.at[0, t, h])

    def add_a(s, t, k, first=False):
        d = dot_nt(gx[s, 0], qt[k, t, 0]) + dot_nt(gx[s, 1], qt[k, t, 1])
        d = (d * inv[t]).astype(BF16).astype(F32)
        acc1[t] = d if first else acc1[t] + d

    def add_b(t, k, first=False):
        d = dot_nt(at[k, 0], dz[k, t, 0]) + dot_nt(at[k, 1], dz[k, t, 1])
        d = (d * inv[t]).astype(BF16).astype(F32)
        acc2[t] = d if first else acc2[t] + d

    start_if(outer, z_e)
    start_if(inner, z_x[2])
    prep(OWN, 0)
    prep(OWN, 1)
    start_if(inner, z_x[3])
    exchange_wait(cnts, ls.at[7])
    total = jnp.sum(cnts[...], axis=0)
    recip = 1.0 / jnp.maximum(total, 1.0)
    for t in range(TASKS):
        inv[t] = jnp.broadcast_to(recip[:, t:t + 1], (1, DIM))
    for t in range(TASKS):
        add_a(OWN, t, 0, True)
        add_b(t, 0, True)
    start_if(inner, z_x[4])
    start_if(outer, z_x[2])
    start_if(outer, z_x[3])
    for cp in (x_e, x_x[0], x_x[1]):
        cp.wait_recv()
    forward(z_x[0], xz_x[0], yz_x[0])
    prep_a(FROM_X, 0, 0)
    start_if(outer, z_x[4])
    forward(z_e, xz_e, yz_e)
    forward(z_x[1], xz_x[1], yz_x[1])
    prep_a(FROM_X, 1, 0)
    for t in range(TASKS):
        add_a(FROM_X, t, 0)
    for cp in (y_e, y_x[0], y_x[1]):
        cp.wait_recv()
    prep_b(FROM_Y, 0, 0)
    prep_b(FROM_Y, 1, 0)
    for t in range(TASKS):
        add_b(t, 0)
    forward(z_x[2], xz_x[2], yz_x[2])
    prep(FROM_Z, 0)
    forward(z_x[3], xz_x[3], yz_x[3])
    forward(z_x[4], xz_x[4], yz_x[4])
    prep(FROM_Z, 1)
    for cp in (xz_e, xz_x[0], xz_x[1]):
        cp.wait_recv()
    prep_a(FROM_XZ, 0, 1)
    for cp in (yz_e, yz_x[0], yz_x[1]):
        cp.wait_recv()
    prep_b(FROM_YZ, 0, 1)
    add_a(FROM_Z, 0, 0)
    for cp in xz_x[2:]:
        cp.wait_recv()

    def rows(base, n):
        return pl.ds(pl.multiple_of(base, 8), n)
    bits1, bits2 = (c, y, e), (c, x, e)
    dest1, dest2 = (to_c, to_y, to_zl), (to_c, to_x, to_zl)

    def moves(bits, u, stage):
        bc, bm, be = bits

        def pick(at0, b, n):
            return at0 + n * (1 - b), at0 + n * b, n
        at0 = 192 * u
        if stage == 0:
            return pick(at0, bc, 96)
        at0 = at0 + 96 * bc
        if stage == 1:
            return pick(at0, bm, 48)
        return pick(at0 + 48 * bm, be, 24)

    part1 = (acc1, (rc1, ra1, rb1), bits1, dest1)
    part2 = (acc2, (rc2, ra2, rb2), bits2, dest2)
    order = [(t, u) for t in range(TASKS) for u in range(2)]
    cps = {}

    def go(part, i, t, u, stage):
        acc, recv, bits, dest = part
        out, _, n = moves(bits, u, stage)
        cps[i, t, u, stage] = start(
            rcopy(acc.at[t, rows(out, n)], recv[stage].at[t, u], dest[stage], 2 * stage + i + 1))

    def merge(part, t, u, stage):
        acc, recv, bits, _ = part
        _, kept, n = moves(bits, u, stage)
        v = acc[t, rows(kept, n)] + recv[stage][t, u]
        acc[t, rows(kept, n)] = v
        return v

    def add(part, i, t, u, stage):
        cps[i, t, u, stage].wait_recv()
        return merge(part, t, u, stage)

    own = 2 * zh + x
    fx, fz = flip(x), 2 * flip(zh)
    back = []

    for part in (pl.ds(0, 24), pl.ds(24, 16)):
        for dk, to in ((fz, to_zh), (fx + fz, to_x + to_zh - me), (fx, to_x)):
            back.append(rcopy(sb.at[own + dk, part], rb.at[own, part], to, 8))

    def send_back(which, cond):
        @pl.when(cond)
        def _():
            for cp in back[3 * which:3 * which + 3]:
                cp.start()

    def finish(t, u):
        g = add(part1, 1, t, u, 2)
        g1s[t, tile(u, 24)] = g
        for k in range(2):
            sb[2 * u + k, tile(t, 12)] = g[tile(k, 12)]
        g2s[t, tile(u, 24)] = add(part2, 2, t, u, 2)

    both = ((1, part1), (2, part2))

    def first_hop(n):
        for i, part in both:
            add(part, i, *order[n], 0)
            go(part, i, *order[n], 1)

    slope(FROM_XZ, 1)
    for t in range(TASKS):
        dz_of(FROM_XZ, 1, t, dzx)
        q_of(1, t, 1, dzx)
        if t:
            add_a(FROM_Z, t, 0)
        add_a(FROM_XZ, t, 1)
        for u in range(2):
            go(part1, 1, t, u, 0)
        if t:
            first_hop(2 * t - 2)
        if t == 0:
            for cp in yz_x[2:]:
                cp.wait_recv()
            act(FROM_YZ, 1, 1)
        dz_of(FROM_YZ, 1, t, dz.at[1, t, 1])
        add_b(t, 0)
        add_b(t, 1)
        for u in range(2):
            go(part2, 2, t, u, 0)
        if t == 1:
            first_hop(1)
    sb[:, 36:40, :] = jnp.zeros((4, 4, DIM), F32)
    for n in range(6):
        if n + 3 < 6:
            for i, part in both:
                add(part, i, *order[n + 3], 0)
        for i, part in both:
            cps[i, *order[n], 1].wait_recv()
            if n + 3 < 6:
                go(part, i, *order[n + 3], 1)
            merge(part, *order[n], 1)
            go(part, i, *order[n], 2)
        if n >= 2:
            finish(*order[n - 2])
    send_back(0, inner)
    finish(*order[4])
    send_back(0, outer)
    finish(*order[5])

    row = jnp.zeros((1, 128), F32)
    pairs = [(t, s) for t in range(TASKS) for s in range(t, TASKS)]
    for i, (t, s) in enumerate(pairs):
        part = jnp.sum(g1s[t] * g1s[s] + g2s[t] * g2s[s], axis=0, keepdims=True)
        row = row + jnp.where(lane == i, jnp.sum(part, axis=1, keepdims=True), 0.0)
    grams[me] = row
    exchange_start(grams, ls.at[8], ls.at[9])
    for cp in back[3:]:
        cp.start()
    rb[own] = sb[own]
    for t in range(TASKS):
        for k in range(3):
            o2_ref[t, pl.ds(k, 48, stride=3), :] = g2s[t, :, tile(k)]
    for cp in back:
        cp.wait_recv()
    for t in range(TASKS):
        parts = []
        for b in range(32):
            bc, bx, by, bzl, bzh = (bit(b, i) for i in range(5))
            at0 = 192 * bc + 96 * (bzl ^ bzh) + 48 * by
            parts.append(rb[2 * bzh + bx, tile(t, 12), at0:at0 + 48])
        full = jnp.concatenate(parts, axis=1)
        for k in range(12):
            o1_ref[t, pl.ds(k, 12, stride=12), :] = full[:, tile(k)]
    exchange_wait(grams, ls.at[9])
    m = jnp.sum(grams[...], axis=0)
    ent = [jnp.broadcast_to(m[:, i:i + 1], (8, 128)) for i in range(6)]
    neg = -TASKS / sum(ent[i] for i, (t, s) in enumerate(pairs) if t == s)
    gram = {}
    for i, (t, s) in enumerate(pairs):
        gram[t, s] = gram[s, t] = ent[i] * neg
    w = [jnp.full((8, 128), 1.0 / TASKS, F32)] * TASKS
    for _ in range(SOLVER_STEPS):
        up = [w[t] * jnp.exp(sum(gram[t, s] * w[s] for s in range(TASKS))) for t in range(TASKS)]
        norm = 1.0 / sum(up)
        w = [v * norm for v in up]
    al_ref[...] = sum(jnp.where(lane == t, w[t][:1], 0.0) for t in range(TASKS))[:, :TASKS]
    exchange_wait(cnts, ls.at[6])
    exchange_wait(grams, ls.at[8])
    for i, ref in enumerate((gx.at[pl.ds(0, 5)], ge.at[pl.ds(0, 5)], rc1, rc2, ra1, ra2, rb1, rb2, rb.at[pl.ds(0, 3)])):
        wait_bytes(ref, ss.at[i])


def solution(mesh):
    def step(tokens, w_in, w_out, heads, lab, msk):
        vm = pl.BlockSpec(memory_space=pltpu.VMEM)
        dma = pltpu.SemaphoreType.DMA
        v = pltpu.VMEM
        alpha, g1, g2 = pl.pallas_call(
            kernel,
            name="step",
            out_shape=(jax.ShapeDtypeStruct((1, TASKS), F32), jax.ShapeDtypeStruct((TASKS, 144, 128), F32),
                       jax.ShapeDtypeStruct((TASKS, 144, 128), F32)),
            in_specs=[pl.BlockSpec(memory_space=pltpu.HBM)] * 6,
            out_specs=(vm, vm, vm),
            scratch_shapes=[
                v((TOK, DIM), BF16), v((DIM, HID), BF16), v((HID, DIM), BF16),
                v((TASKS, CLS, DIM), BF16), v((TASKS, TOK), jnp.int32),
                v((TASKS, TOK), jnp.int32), v((TASKS * PAD, DIM), BF16),
                v((N_DEV, 1, 128), F32), v((N_DEV, 1, 128), F32),
                v((6, 2, DIM, HALF), BF16), v((6, TASKS, PAD, TOK), BF16),
                v((TASKS, DIM, PAD), BF16), v((DIM, DIM), BF16), v((DIM, DIM), BF16), v((DIM, DIM), BF16),
                v((TOK, HID), BF16), v((2, 2, DIM, HALF), BF16), v((DIM, HALF), F32),
                v((2, TASKS, 2, DIM, HALF), BF16), v((DIM, HALF), BF16), v((2, TASKS, 2, DIM, HALF), BF16),
                v((TASKS, 1, DIM), F32),
                v((TASKS, DIM, DIM), F32), v((TASKS, DIM, DIM), F32),
                v((TASKS, 2, 96, DIM), F32), v((TASKS, 2, 96, DIM), F32),
                v((TASKS, 2, 48, DIM), F32), v((TASKS, 2, 48, DIM), F32),
                v((TASKS, 2, 24, DIM), F32), v((TASKS, 2, 24, DIM), F32),
                v((TASKS, 48, DIM), F32), v((TASKS, 48, DIM), F32),
                v((4, 40, DIM), F32), v((4, 40, DIM), F32),
                dma((9,)), dma((N_SEM,)), dma((10,)),
            ],
            compiler_params=pltpu.CompilerParams(collective_id=0, has_side_effects=True, vmem_limit_bytes=28 * 2**20),
        )(*[pltpu.with_memory_space_constraint(a, pltpu.HBM)
            for a in (tokens, w_in, w_out, heads.transpose(0, 2, 1), lab, msk)])
        alpha = alpha.reshape(TASKS)
        w = alpha[:, None, None]
        return alpha, (w * g1).sum(axis=0).reshape(-1), (w * g2).sum(axis=0).reshape(-1)

    return jax.shard_map(step, mesh=mesh, in_specs=(P("data", None), P(), P(), P(), P(None, "data"), P(None, "data")),
                         out_specs=(P(), P("data"), P("data")), check_vma=False)
```

```python
import jax
import jax.numpy as jnp
from jax import lax
from jax.experimental import pallas as pl
from jax.experimental.pallas import tpu as pltpu
from jax.sharding import PartitionSpec as P

MESH = pl.DeviceIdType.MESH
SOLVER_STEPS = 20
N_DEV = 32
TOK, DIM, HID, TASKS, CLS, PAD = 512, 384, 1536, 3, 13, 16
HALF = TOK // 2
GELU_C = 0.7978845608028654
GELU_A = 0.044715
N_SEM = 66
OWN, FROM_X, FROM_Z, FROM_XZ, FROM_Y, FROM_YZ = range(6)

F32, BF16 = jnp.float32, jnp.bfloat16


def dot(a, b):
    return jnp.dot(a, b, preferred_element_type=F32)


def dot_nt(a, b):
    return lax.dot_general(a, b, (((1,), (1,)), ((), ())), preferred_element_type=F32)


def bit(v, i):
    return (v >> i) & 1


def flip(b):
    return 1 - 2 * b


def index(c, x, y, zl, zh):
    return c + 2 * x + 4 * y + 8 * zl + 16 * zh


def tile(k, n=128):
    return slice(n * k, n * (k + 1))


def gelu_cdf(p):
    sq = p * p
    t = jnp.tanh(GELU_C * (p + GELU_A * (sq * p)))
    return sq, t, 0.5 * (1.0 + t)


def kernel(x_hbm, w1_hbm, w2_hbm, h_hbm, lab_hbm, msk_hbm, al_ref, o1_ref, o2_ref,
           x_ref, w1_ref, w2_ref, h_ref, lab_ref, msk_ref, hp_ref, cnts, grams,
           gx, ge, ht, w1a, w1b, w2a, a_own, at, gp, dz, dzx, qt, inv, acc1, acc2,
           rc1, rc2, ra1, ra2, rb1, rb2, g1s, g2s, sb, rb,
           ss, rs, ls):
    me = lax.axis_index("data")
    c, x, y, zl, zh = (lax.rem(me // n, 2) for n in (1, 2, 4, 8, 16))
    to_c, to_x, to_y = me + flip(c), me + 2 * flip(x), me + 4 * flip(y)
    to_zh = me + index(0, 0, 0, flip(zl), flip(zh))
    e = lax.rem(zh + zl, 2)
    to_zl = me + 8 * flip(zl)

    used = []

    def rcopy(src, dst, dev, group):
        i = len(used)
        used.append(i)
        return pltpu.make_async_remote_copy(src_ref=src, dst_ref=dst, send_sem=ss.at[group], recv_sem=rs.at[i],
                                            device_id=(dev,), device_id_type=MESH)

    def start(cp):
        cp.start()
        return cp

    def wait_bytes(ref, sem):
        pltpu.make_async_copy(ref, ref, sem).wait()

    def row_copy(buf, src_row, send_sem, recv_sem, dev):
        return pltpu.make_async_remote_copy(src_ref=buf.at[src_row], dst_ref=buf.at[src_row], send_sem=send_sem,
                                            recv_sem=recv_sem, device_id=(dev,), device_id_type=MESH)

    def exchange_start(buf, s_sem, r_sem):
        def go(i, _):
            row_copy(buf, me, s_sem, r_sem, lax.rem(me + i, N_DEV)).start()
            return 0
        lax.fori_loop(1, N_DEV, go, 0, unroll=True)

    def exchange_wait(buf, sem):
        wait_bytes(buf.at[pl.ds(0, N_DEV - 1)], sem)

    loads = [pltpu.make_async_copy(a, b, ls.at[i]) for i, (a, b) in enumerate((
        (x_hbm, x_ref), (msk_hbm, msk_ref), (w1_hbm, w1_ref), (w2_hbm, w2_ref), (h_hbm, h_ref), (lab_hbm, lab_ref)))]
    for cp in loads:
        cp.start()

    bar = pltpu.get_barrier_semaphore()

    def sig(i, _):
        pl.semaphore_signal(bar, inc=1, device_id=(lax.rem(me + i, N_DEV),), device_id_type=MESH)
        return 0
    lax.fori_loop(1, N_DEV, sig, 0)

    col = lax.broadcasted_iota(jnp.int32, (DIM, 1), 0)
    blk = (col * 43691) >> 19
    dev = index(bit(blk, 3), bit(blk, 0), bit(blk, 2), bit(blk, 1) ^ bit(blk, 4), bit(blk, 4))
    perm = (lax.broadcasted_iota(jnp.int32, (DIM, DIM), 1) == 12 * dev + (col - 12 * blk)).astype(BF16)
    loads[0].wait()
    for h in range(2):
        gx[OWN, h] = dot_nt(perm, x_ref[tile(h, HALF), :]).astype(BF16)
    lane = lax.broadcasted_iota(jnp.int32, (1, 128), 1)
    row = jnp.zeros((1, 128), F32)
    loads[1].wait()
    for t in range(TASKS):
        row = row + jnp.where(lane == t, jnp.sum(msk_ref[t:t + 1, :].astype(F32), axis=1, keepdims=True), 0.0)
    cnts[me] = row

    pl.semaphore_wait(bar, N_DEV - 1)

    def piece(slot, h, r0=0, n=DIM):
        return gx.at[slot, h, pl.ds(r0, n)]
    cuts = ((0, 0, 192), (0, 192, 192), (1, 0, 192), (1, 192, 96), (1, 288, 96))
    z_x = [rcopy(piece(OWN, *k), piece(FROM_Z, *k), to_zh, 0) for k in cuts]
    x_x = [rcopy(piece(OWN, h), piece(FROM_X, h), to_x, 0) for h in range(2)]
    y_x = [rcopy(piece(OWN, h), piece(FROM_Y, h), to_y, 0) for h in range(2)]
    xz_x = [rcopy(piece(FROM_Z, *k), piece(FROM_XZ, *k), to_x, 0) for k in cuts]
    yz_x = [rcopy(piece(FROM_Z, *k), piece(FROM_YZ, *k), to_y, 0) for k in cuts]
    z_e = rcopy(ge.at[OWN], ge.at[FROM_Z], to_zh, 1)
    x_e = rcopy(ge.at[OWN], ge.at[FROM_X], to_x, 1)
    y_e = rcopy(ge.at[OWN], ge.at[FROM_Y], to_y, 1)
    xz_e = rcopy(ge.at[FROM_Z], ge.at[FROM_XZ], to_x, 1)
    yz_e = rcopy(ge.at[FROM_Z], ge.at[FROM_YZ], to_y, 1)

    outer, inner = e == 0, e == 1

    def start_if(cond, cp):
        @pl.when(cond)
        def _():
            cp.start()

    def forward(got, a, b):
        got.wait_recv()
        start(a)
        start(b)

    exchange_start(cnts, ls.at[6], ls.at[7])
    start(z_x[0])
    start(x_x[0])
    start(y_x[0])

    for cp in loads[2:]:
        cp.wait()
    hp_ref[...] = jnp.zeros_like(hp_ref)
    for t in range(TASKS):
        hp_ref[PAD * t:PAD * t + CLS, :] = h_ref[t]

    def fwd(i, _):
        cols = pl.ds(pl.multiple_of(i * 256, 256), 256)
        p = dot(x_ref[...], w1_ref[:, cols])
        a_own[:, cols] = (p * gelu_cdf(p)[2]).astype(BF16)
        return 0
    lax.fori_loop(0, HID // 256, fwd, 0)
    start_if(inner, z_x[1])
    z = (x_ref[...].astype(F32) + dot(a_own[...], w2_ref[...])).astype(BF16)
    logits = dot_nt(hp_ref[...], z)
    cls = lax.broadcasted_iota(jnp.int32, (PAD, TOK), 0)
    valid = cls < CLS
    for t in range(TASKS):
        lg = jnp.where(valid, logits[tile(t, PAD)], -jnp.inf)
        ex = jnp.exp(lg - jnp.max(lg, axis=0, keepdims=True))
        sm = ex / jnp.sum(ex, axis=0, keepdims=True)
        hot = (lab_ref[t:t + 1, :] == cls).astype(F32)
        ge[OWN, t] = jnp.where(valid, msk_ref[t:t + 1, :].astype(F32) * (sm - hot), 0.0).astype(BF16)
    start_if(inner, z_e)
    start_if(outer, z_x[1])
    start(x_e)
    start(y_e)
    start(x_x[1])
    start(y_x[1])

    hid_iota = lax.broadcasted_iota(jnp.int32, (DIM, HID), 1)
    seg = (col * 43691) >> 21
    src_a = 48 * (index(bit(seg, 2), x, bit(seg, 0), bit(seg, 1) ^ zh, zh) - seg) + col
    seg = (col * 43691) >> 20
    src_b = 48 * index(bit(seg, 2), bit(seg, 1), y, bit(seg, 0) ^ zh, zh) + 24 * (bit(seg, 3) - seg) + col
    for src, dst in ((src_a, w1a), (src_b, w1b)):
        sel = (hid_iota == src).astype(BF16)
        dst[...] = dot_nt(dot_nt(sel, w1_ref[...]).astype(BF16), perm).astype(BF16)
    for k in range(8):
        dv = index(bit(k, 2), x, bit(k, 0), bit(k, 1) * flip(zh) + zh, zh)
        w2a[tile(k, 48), :] = w2_ref[pl.ds(pl.multiple_of(48 * dv, 16), 48), :]
    for t in range(TASKS):
        ht[t] = jnp.transpose(hp_ref[tile(t, PAD), :].astype(F32)).astype(BF16)

    strips = [tile(r) for r in range(TASKS)]

    def slope(s, h):
        for rows in strips:
            p = dot(w1a[rows, :], gx[s, h])
            sq, t, cdf = gelu_cdf(p)
            gp[rows, :] = cdf + (0.5 * GELU_C) * p * (1.0 - t * t) * (1.0 + (3.0 * GELU_A) * sq)

    def act(s, h, k):
        for rows in strips:
            p = dot(w1b[rows, :], gx[s, h])
            at[k, h, rows, :] = (p * gelu_cdf(p)[2]).astype(BF16)

    def dz_of(s, h, t, ref):
        ref[...] = dot(ht[t], ge[s, t, :, tile(h, HALF)]).astype(BF16)

    def q_of(h, t, k, ref):
        for rows in strips:
            qt[k, t, h, rows, :] = (dot(w2a[rows, :], ref[...]) * gp[rows, :]).astype(BF16)

    def prep_a(s, h, k):
        slope(s, h)
        for t in range(TASKS):
            dz_of(s, h, t, dzx)
            q_of(h, t, k, dzx)

    def prep_b(s, h, k):
        act(s, h, k)
        for t in range(TASKS):
            dz_of(s, h, t, dz.at[k, t, h])

    def prep(s, h):
        slope(s, h)
        act(s, h, 0)
        for t in range(TASKS):
            dz_of(s, h, t, dz.at[0, t, h])
            q_of(h, t, 0, dz.at[0, t, h])

    def add_a(s, t, k, first=False):
        d = dot_nt(gx[s, 0], qt[k, t, 0]) + dot_nt(gx[s, 1], qt[k, t, 1])
        d = (d * inv[t]).astype(BF16).astype(F32)
        acc1[t] = d if first else acc1[t] + d

    def add_b(t, k, first=False):
        d = dot_nt(at[k, 0], dz[k, t, 0]) + dot_nt(at[k, 1], dz[k, t, 1])
        d = (d * inv[t]).astype(BF16).astype(F32)
        acc2[t] = d if first else acc2[t] + d

    start_if(outer, z_e)
    start_if(inner, z_x[2])
    prep(OWN, 0)
    prep(OWN, 1)
    start_if(inner, z_x[3])
    exchange_wait(cnts, ls.at[7])
    total = jnp.sum(cnts[...], axis=0)
    recip = 1.0 / jnp.maximum(total, 1.0)
    for t in range(TASKS):
        inv[t] = jnp.broadcast_to(recip[:, t:t + 1], (1, DIM))
    for t in range(TASKS):
        add_a(OWN, t, 0, True)
        add_b(t, 0, True)
    start_if(inner, z_x[4])
    start_if(outer, z_x[2])
    start_if(outer, z_x[3])
    for cp in (x_e, x_x[0], x_x[1]):
        cp.wait_recv()
    forward(z_x[0], xz_x[0], yz_x[0])
    prep_a(FROM_X, 0, 0)
    start_if(outer, z_x[4])
    forward(z_e, xz_e, yz_e)
    forward(z_x[1], xz_x[1], yz_x[1])
    prep_a(FROM_X, 1, 0)
    for t in range(TASKS):
        add_a(FROM_X, t, 0)
    for cp in (y_e, y_x[0], y_x[1]):
        cp.wait_recv()
    prep_b(FROM_Y, 0, 0)
    prep_b(FROM_Y, 1, 0)
    for t in range(TASKS):
        add_b(t, 0)
    forward(z_x[2], xz_x[2], yz_x[2])
    prep(FROM_Z, 0)
    forward(z_x[3], xz_x[3], yz_x[3])
    forward(z_x[4], xz_x[4], yz_x[4])
    prep(FROM_Z, 1)
    for cp in (xz_e, xz_x[0], xz_x[1]):
        cp.wait_recv()
    prep_a(FROM_XZ, 0, 1)
    for cp in (yz_e, yz_x[0], yz_x[1]):
        cp.wait_recv()
    prep_b(FROM_YZ, 0, 1)
    add_a(FROM_Z, 0, 0)
    for cp in xz_x[2:]:
        cp.wait_recv()

    def rows(base, n):
        return pl.ds(pl.multiple_of(base, 8), n)
    bits1, bits2 = (c, y, e), (c, x, e)
    dest1, dest2 = (to_c, to_y, to_zl), (to_c, to_x, to_zl)

    def moves(bits, u, stage):
        bc, bm, be = bits

        def pick(at0, b, n):
            return at0 + n * (1 - b), at0 + n * b, n
        at0 = 192 * u
        if stage == 0:
            return pick(at0, bc, 96)
        at0 = at0 + 96 * bc
        if stage == 1:
            return pick(at0, bm, 48)
        return pick(at0 + 48 * bm, be, 24)

    part1 = (acc1, (rc1, ra1, rb1), bits1, dest1)
    part2 = (acc2, (rc2, ra2, rb2), bits2, dest2)
    order = [(t, u) for t in range(TASKS) for u in range(2)]
    cps = {}

    def go(part, i, t, u, stage):
        acc, recv, bits, dest = part
        out, _, n = moves(bits, u, stage)
        cps[i, t, u, stage] = start(
            rcopy(acc.at[t, rows(out, n)], recv[stage].at[t, u], dest[stage], 2 * stage + i + 1))

    def merge(part, t, u, stage):
        acc, recv, bits, _ = part
        _, kept, n = moves(bits, u, stage)
        v = acc[t, rows(kept, n)] + recv[stage][t, u]
        acc[t, rows(kept, n)] = v
        return v

    def add(part, i, t, u, stage):
        cps[i, t, u, stage].wait_recv()
        return merge(part, t, u, stage)

    own = 2 * zh + x
    fx, fz = flip(x), 2 * flip(zh)
    back = []

    for part in (pl.ds(0, 24), pl.ds(24, 16)):
        for dk, to in ((fz, to_zh), (fx + fz, to_x + to_zh - me), (fx, to_x)):
            back.append(rcopy(sb.at[own + dk, part], rb.at[own, part], to, 8))

    def send_back(which, cond):
        @pl.when(cond)
        def _():
            for cp in back[3 * which:3 * which + 3]:
                cp.start()

    def finish(t, u):
        g = add(part1, 1, t, u, 2)
        g1s[t, tile(u, 24)] = g
        for k in range(2):
            sb[2 * u + k, tile(t, 12)] = g[tile(k, 12)]
        g2s[t, tile(u, 24)] = add(part2, 2, t, u, 2)

    both = ((1, part1), (2, part2))

    def first_hop(n):
        for i, part in both:
            add(part, i, *order[n], 0)
            go(part, i, *order[n], 1)

    slope(FROM_XZ, 1)
    for t in range(TASKS):
        dz_of(FROM_XZ, 1, t, dzx)
        q_of(1, t, 1, dzx)
        if t:
            add_a(FROM_Z, t, 0)
        add_a(FROM_XZ, t, 1)
        for u in range(2):
            go(part1, 1, t, u, 0)
        if t:
            first_hop(2 * t - 2)
        if t == 0:
            for cp in yz_x[2:]:
                cp.wait_recv()
            act(FROM_YZ, 1, 1)
        dz_of(FROM_YZ, 1, t, dz.at[1, t, 1])
        add_b(t, 0)
        add_b(t, 1)
        for u in range(2):
            go(part2, 2, t, u, 0)
        if t == 1:
            first_hop(1)
    sb[:, 36:40, :] = jnp.zeros((4, 4, DIM), F32)
    for n in range(6):
        if n + 3 < 6:
            for i, part in both:
                add(part, i, *order[n + 3], 0)
        for i, part in both:
            cps[i, *order[n], 1].wait_recv()
            if n + 3 < 6:
                go(part, i, *order[n + 3], 1)
            merge(part, *order[n], 1)
            go(part, i, *order[n], 2)
        if n >= 2:
            finish(*order[n - 2])
    send_back(0, inner)
    finish(*order[4])
    send_back(0, outer)
    finish(*order[5])

    row = jnp.zeros((1, 128), F32)
    pairs = [(t, s) for t in range(TASKS) for s in range(t, TASKS)]
    for i, (t, s) in enumerate(pairs):
        part = jnp.sum(g1s[t] * g1s[s] + g2s[t] * g2s[s], axis=0, keepdims=True)
        row = row + jnp.where(lane == i, jnp.sum(part, axis=1, keepdims=True), 0.0)
    grams[me] = row
    exchange_start(grams, ls.at[8], ls.at[9])
    for cp in back[3:]:
        cp.start()
    rb[own] = sb[own]
    for t in range(TASKS):
        for k in range(3):
            o2_ref[t, pl.ds(k, 48, stride=3), :] = g2s[t, :, tile(k)]
    for cp in back:
        cp.wait_recv()
    for t in range(TASKS):
        parts = []
        for b in range(32):
            bc, bx, by, bzl, bzh = (bit(b, i) for i in range(5))
            at0 = 192 * bc + 96 * (bzl ^ bzh) + 48 * by
            parts.append(rb[2 * bzh + bx, tile(t, 12), at0:at0 + 48])
        full = jnp.concatenate(parts, axis=1)
        for k in range(12):
            o1_ref[t, pl.ds(k, 12, stride=12), :] = full[:, tile(k)]
    exchange_wait(grams, ls.at[9])
    m = jnp.sum(grams[...], axis=0)
    ent = [jnp.broadcast_to(m[:, i:i + 1], (8, 128)) for i in range(6)]
    neg = -TASKS / sum(ent[i] for i, (t, s) in enumerate(pairs) if t == s)
    gram = {}
    for i, (t, s) in enumerate(pairs):
        gram[t, s] = gram[s, t] = ent[i] * neg
    w = [jnp.full((8, 128), 1.0 / TASKS, F32)] * TASKS
    for _ in range(SOLVER_STEPS):
        up = [w[t] * jnp.exp(sum(gram[t, s] * w[s] for s in range(TASKS))) for t in range(TASKS)]
        norm = 1.0 / sum(up)
        w = [v * norm for v in up]
    al_ref[...] = sum(jnp.where(lane == t, w[t][:1], 0.0) for t in range(TASKS))[:, :TASKS]
    exchange_wait(cnts, ls.at[6])
    exchange_wait(grams, ls.at[8])
    for i, ref in enumerate((gx.at[pl.ds(0, 5)], ge.at[pl.ds(0, 5)], rc1, rc2, ra1, ra2, rb1, rb2, rb.at[pl.ds(0, 3)])):
        wait_bytes(ref, ss.at[i])


def solution(mesh):
    def step(tokens, w_in, w_out, heads, lab, msk):
        vm = pl.BlockSpec(memory_space=pltpu.VMEM)
        dma = pltpu.SemaphoreType.DMA
        v = pltpu.VMEM
        alpha, g1, g2 = pl.pallas_call(
            kernel,
            name="step",
            out_shape=(jax.ShapeDtypeStruct((1, TASKS), F32), jax.ShapeDtypeStruct((TASKS, 144, 128), F32),
                       jax.ShapeDtypeStruct((TASKS, 144, 128), F32)),
            in_specs=[pl.BlockSpec(memory_space=pltpu.HBM)] * 6,
            out_specs=(vm, vm, vm),
            scratch_shapes=[
                v((TOK, DIM), BF16), v((DIM, HID), BF16), v((HID, DIM), BF16),
                v((TASKS, CLS, DIM), BF16), v((TASKS, TOK), jnp.int32),
                v((TASKS, TOK), jnp.int32), v((TASKS * PAD, DIM), BF16),
                v((N_DEV, 1, 128), F32), v((N_DEV, 1, 128), F32),
                v((6, 2, DIM, HALF), BF16), v((6, TASKS, PAD, TOK), BF16),
                v((TASKS, DIM, PAD), BF16), v((DIM, DIM), BF16), v((DIM, DIM), BF16), v((DIM, DIM), BF16),
                v((TOK, HID), BF16), v((2, 2, DIM, HALF), BF16), v((DIM, HALF), F32),
                v((2, TASKS, 2, DIM, HALF), BF16), v((DIM, HALF), BF16), v((2, TASKS, 2, DIM, HALF), BF16),
                v((TASKS, 1, DIM), F32),
                v((TASKS, DIM, DIM), F32), v((TASKS, DIM, DIM), F32),
                v((TASKS, 2, 96, DIM), F32), v((TASKS, 2, 96, DIM), F32),
                v((TASKS, 2, 48, DIM), F32), v((TASKS, 2, 48, DIM), F32),
                v((TASKS, 2, 24, DIM), F32), v((TASKS, 2, 24, DIM), F32),
                v((TASKS, 48, DIM), F32), v((TASKS, 48, DIM), F32),
                v((4, 40, DIM), F32), v((4, 40, DIM), F32),
                dma((9,)), dma((N_SEM,)), dma((10,)),
            ],
            compiler_params=pltpu.CompilerParams(collective_id=0, has_side_effects=True, vmem_limit_bytes=28 * 2**20),
        )(*[pltpu.with_memory_space_constraint(a, pltpu.HBM)
            for a in (tokens, w_in, w_out, heads.transpose(0, 2, 1), lab, msk)])
        alpha = alpha.reshape(TASKS)
        w = alpha[:, None, None]
        return alpha, (w * g1).sum(axis=0).reshape(-1), (w * g2).sum(axis=0).reshape(-1)

    return jax.shard_map(step, mesh=mesh, in_specs=(P("data", None), P(), P(), P(), P(None, "data"), P(None, "data")),
                         out_specs=(P(), P("data"), P("data")), check_vma=False)
```
